32 devices in a mesh: col: 4 (over z), row: 8 (over y, x, core).
Axes of the slice: x: 2, y: 2, z: 4, core: 2. Of those that a mesh axis runs over, the one named last changes fastest.
Arguments:
- psi_init: float32 [2048, 2, 2048], P('row', None, 'col')
- left_env: float32 [2048, 14, 2048], P('row')
- mpo_tensor: float32 [14, 14, 2, 2], replicated
- right_env: float32 [2048, 14, 2048], P('col')
Outputs:
- output 1: float32 [4], replicated
- output 2: float32 [4], replicated
- output 3: float32 [2048, 2, 2048], P('row', None, 'col')
All inputs are finite; a program needn't handle non-finite values.
Results may differ from the reference program's by a relative error of at most 0.001.
Values sent between devices are 32-bit elements.
A program may use at most 1 GiB of HBM per device.

```python
import jax
import jax.numpy as jnp
from jax import lax

BOND_DIM = 2048
PHYS_DIM = 2
MPO_DIM = 14
LANCZOS_STEPS = 4
REF_BLOCK = min(BOND_DIM, 128)
EXACT_PREC = lax.Precision.HIGHEST


def make_env(key_dense, key_shift):
    dense_part = jax.random.normal(key_dense, (BOND_DIM, MPO_DIM, BOND_DIM), jnp.float32)
    dense_part = (dense_part + jnp.transpose(dense_part, (2, 1, 0))) * (0.5 / BOND_DIM) ** 0.5
    shifts = 1.0 + 0.5 * jax.random.normal(key_shift, (MPO_DIM,), jnp.float32)
    eye_mat = jnp.eye(BOND_DIM, dtype=jnp.float32)
    return dense_part + eye_mat[:, None, :] * shifts[None, :, None]


def setup_inputs(seed: int = 0) -> dict:
    key_list = jax.random.split(jax.random.key(seed), 6)
    psi_init = jax.random.normal(key_list[0], (BOND_DIM, PHYS_DIM, BOND_DIM), jnp.float32)
    left_env = make_env(key_list[1], key_list[2])
    mpo_raw = jax.random.normal(key_list[3], (MPO_DIM, MPO_DIM, PHYS_DIM, PHYS_DIM), jnp.float32)
    mpo_tensor = (mpo_raw + jnp.transpose(mpo_raw, (0, 1, 3, 2))) * (0.5 ** 0.5 / (MPO_DIM * PHYS_DIM ** 0.5))
    mpo_tensor = mpo_tensor + jnp.eye(PHYS_DIM, dtype=jnp.float32) / MPO_DIM ** 2
    right_env = make_env(key_list[4], key_list[5])
    return {"psi_init": psi_init, "left_env": left_env, "mpo_tensor": mpo_tensor, "right_env": right_env}


def apply_ham(vec_in, left_blocks, mpo_tensor, right_env):
    def one_block(left_blk):
        t_one = jnp.einsum("alc,asb->lcsb", left_blk, vec_in, precision=EXACT_PREC)
        t_two = jnp.einsum("lcsb,lrst->cbrt", t_one, mpo_tensor, precision=EXACT_PREC)
        return jnp.einsum("cbrt,brd->ctd", t_two, right_env, precision=EXACT_PREC)
    out_blocks = lax.map(one_block, left_blocks)
    return out_blocks.reshape(BOND_DIM, PHYS_DIM, BOND_DIM)


def reference(psi_init, left_env, mpo_tensor, right_env):
    block_count = BOND_DIM // REF_BLOCK
    left_blocks = jnp.transpose(left_env.reshape(BOND_DIM, MPO_DIM, block_count, REF_BLOCK), (2, 0, 1, 3))
    vec_init = psi_init / jnp.sqrt(jnp.sum(psi_init * psi_init))

    def lanczos_step(loop_state, step_input):
        vec_prev, vec_cur, beta_prev = loop_state
        work_vec = apply_ham(vec_cur, left_blocks, mpo_tensor, right_env)
        alpha_val = jnp.sum(vec_cur * work_vec)
        work_vec = work_vec - alpha_val * vec_cur - beta_prev * vec_prev
        beta_val = jnp.sqrt(jnp.sum(work_vec * work_vec))
        return (vec_cur, work_vec / beta_val, beta_val), (alpha_val, beta_val)

    state_init = (jnp.zeros_like(vec_init), vec_init, jnp.zeros((), vec_init.dtype))
    final_state, scalar_lists = lax.scan(lanczos_step, state_init, None, length=LANCZOS_STEPS)
    return scalar_lists[0], scalar_lists[1], final_state[1]
```

```python
import functools

import jax
import jax.numpy as jnp
from jax import lax
from jax.experimental import pallas as pl
from jax.experimental.pallas import tpu as pltpu
from jax.sharding import PartitionSpec as P

F32, BF16 = jnp.float32, jnp.bfloat16
STEPS = 4
NROW, NCOL = 8, 4
NDEV = NROW * NCOL
KRON = 8
PASSES = ((0, 3), (1, 2), (2, 1))


def div(a, b):
    return lax.div(a, jnp.int32(b))


def mod(a, b):
    return lax.rem(a, jnp.int32(b))


def split3(x):
    hi = x.astype(BF16)
    rest = x - hi.astype(F32)
    mid = rest.astype(BF16)
    low = (rest - mid.astype(F32)).astype(BF16)
    return hi, mid, low


def lanczos_kernel(ts, nd, psi, wk, lt, rt, out_v, out_ab,
                   vy, vcur, vprev, wprime, recv, t1, t2, l0, l1, l2, r0, r1, r2, vp, wkp, yacc, ar_src, ar_recv,
                   lsem, rsem, vsend, vrecv, ysend, yrecv, asend, arecv, iosem, fwd_ok, back_ok):
    row, col = lax.axis_index("row"), lax.axis_index("col")
    me = col * NROW + row
    core, xx, yy = mod(row, 2), mod(div(row, 2), 2), div(row, 4)
    per = nd // 2
    hs = ts // 2
    lps, rps = (l0, l1, l2), (r0, r1, r2)

    def six(lhs, rhs):
        a = [x for p, n in PASSES for x in lhs[:n]]
        b = [rhs[p] for p, n in PASSES for _ in range(n)]
        return jnp.dot(jnp.concatenate(a, axis=1), jnp.concatenate(b, axis=0), preferred_element_type=F32)

    def row_of(s):
        fc, fx, fy = mod(s, 2), mod(div(s, 2), 2), div(s, 4)
        c2, x2, y2 = core + fc - 2 * core * fc, xx + fx - 2 * xx * fx, yy + fy - 2 * yy * fy
        return (y2 * 2 + x2) * 2 + c2

    half_z = div(col, 2)
    zdir = 1 - 2 * half_z
    mz = col + half_z * (3 - 2 * col)

    def block_of(i):
        late, two, odd = div(i, 4), div(i, 2), mod(i, 2)
        d_in = (1 - late) * 3 * (1 - odd) + late * (4 - two)
        h_in = (1 - late) * two + late * odd
        return (1 - mz) * (3 - two) + mz * d_in, (1 - mz) * odd + mz * h_in

    def l_batch(g, hh, slot):
        a0 = pl.multiple_of(row_of(g) * ts, ts)
        a1 = pl.multiple_of(row_of(mod(g + hh, 8)) * ts, ts)
        base = per * slot
        if per > 1:
            pltpu.make_async_copy(lt.at[pl.ds(per * hh + 1, per - 1), :, pl.ds(a0, ts)],
                                  recv.at[pl.ds(base, per - 1)], lsem.at[slot]).start()
        pltpu.make_async_copy(lt.at[pl.ds(per - per * hh, 1), :, pl.ds(a1, ts)],
                              recv.at[pl.ds(base + per - 1, 1)], lsem.at[slot]).start()

    def l_batch_wait(slot):
        ref = recv.at[pl.ds(per * slot, per)]
        pltpu.make_async_copy(ref, ref, lsem.at[slot]).wait()

    def r_start(i):
        dm, h = block_of(i)
        dest = dm + half_z * (3 - 2 * dm)
        return pl.multiple_of((dest * 2 + h) * ts, ts)

    def r_batch(i, hh, slot):
        d0, d1 = r_start(i), r_start(mod(i + hh, 8))
        cols = pl.ds(pl.multiple_of(slot * ts, ts), ts)
        if per > 1:
            pltpu.make_async_copy(rt.at[pl.ds(4 * (per * hh + 1), 4 * per - 4), :, pl.ds(d0, ts)],
                                  t1.at[pl.ds(0, 4 * per - 4), pl.ds(0, hs), cols], rsem.at[slot]).start()
        pltpu.make_async_copy(rt.at[pl.ds(4 * (per - per * hh), 4), :, pl.ds(d1, ts)],
                              t1.at[pl.ds(4 * per - 4, 4), pl.ds(0, hs), cols], rsem.at[slot]).start()

    def r_batch_wait(slot):
        ref = t1.at[:, pl.ds(0, hs), pl.ds(pl.multiple_of(slot * ts, ts), ts)]
        pltpu.make_async_copy(ref, ref, rsem.at[slot]).wait()

    def pieces_of(k):
        return 0 if k == 0 else 2 - k % 2

    SB = min(32, ts)

    def l_split(slot, k, dst):
        for b in range(ts // SB):
            rows = pl.ds(b * SB, SB)
            for p, x in enumerate(split3(recv[per * slot + k, rows, :])):
                dst[p, rows, :] = x

    def r_split(slot, k, dst):
        cols = pl.ds(pl.multiple_of(slot * ts, ts), ts)
        sb = min(SB, hs)
        for kb in range(2):
            for bh in range(2):
                for b in range(hs // sb):
                    for p, x in enumerate(split3(t1[4 * k + 2 * kb + bh, pl.ds(b * sb, sb), cols])):
                        dst[p, kb, pl.ds(bh * hs + b * sb, sb), :] = x

    def ar_start(slot, tile):
        ar_src[slot] = tile
        ar_recv[slot, me] = tile

        def send(off, carry):
            to = mod(me + off, NDEV)
            pltpu.make_async_remote_copy(
                src_ref=ar_src.at[slot], dst_ref=ar_recv.at[slot, me], send_sem=asend.at[slot], recv_sem=arecv.at[slot],
                device_id={"col": div(to, NROW), "row": mod(to, NROW)}, device_id_type=pl.DeviceIdType.MESH).start()
            return carry

        lax.fori_loop(1, NDEV, send, 0)

    def ar_wait(slot):
        every = ar_recv.at[slot, pl.ds(0, NDEV - 1)]
        copy = pltpu.make_async_remote_copy(
            src_ref=every, dst_ref=every, send_sem=asend.at[slot], recv_sem=arecv.at[slot],
            device_id={"col": col, "row": row}, device_id_type=pl.DeviceIdType.MESH)
        copy.wait_send()
        copy.wait_recv()
        got = ar_recv[slot]
        first = lax.broadcasted_iota(jnp.int32, got.shape, 1) == 0
        return jnp.sum(jnp.where(first, got, 0.0)), jnp.max(jnp.where(first, 0.0, got))

    RB = min(64, ts)
    nblk = 4 * (ts // RB)

    def where_is(i):
        return div(i, ts // RB), pl.ds(pl.multiple_of(mod(i, ts // RB) * RB, RB), RB)

    def fold(op, x):
        x = x.reshape(RB // 8, 8, ts)
        y = x[0]
        for k in range(1, RB // 8):
            y = op(y, x[k])
        if ts <= 128:
            return y
        return op(y[:, :128], y[:, 128:])

    W8 = min(128, ts)

    def as_row(x, op):
        x = op(x, axis=0, keepdims=True)
        return x if W8 == 128 else jnp.concatenate([x, jnp.zeros((1, 128 - W8), F32)], axis=1)

    def two_rows(a, b):
        first = lax.broadcasted_iota(jnp.int32, (2, 128), 0) == 0
        return jnp.where(first, jnp.broadcast_to(a, (2, 128)), jnp.broadcast_to(b, (2, 128)))

    def vec(x):
        return jnp.full((8, 128), x, F32)

    def scaled_start(src_norm_coef):
        def scale(i, sq):
            n, rows = where_is(i)
            x = wprime[n, rows, :]
            vy[0, n, rows, :] = x * src_norm_coef
            return sq + fold(jnp.add, x * x)

        sq = lax.fori_loop(0, nblk, scale, jnp.zeros((8, W8), F32))
        ar_start(1, two_rows(as_row(sq, jnp.sum), jnp.zeros((1, 128), F32)))

    load = pltpu.make_async_copy(psi, wprime, iosem)
    load.start()
    l_first = pltpu.make_async_copy(lt.at[pl.ds(0, 1), :, pl.ds(pl.multiple_of(row * ts, ts), ts)],
                                    recv.at[pl.ds(2 * per - 1, 1)], lsem.at[1])
    l_first.start()
    r_first = pltpu.make_async_copy(rt.at[pl.ds(0, 4), :, pl.ds(r_start(jnp.int32(0)), ts)],
                                    t1.at[pl.ds(4 * per - 4, 4), pl.ds(0, hs), pl.ds(ts, ts)], rsem.at[1])
    r_first.start()
    zero_i = jnp.int32(0)
    l_batch(zero_i, zero_i, 0)
    for b in range(256 // 32):
        rows = pl.ds(b * 32, 32)
        for p, x in enumerate(split3(wk[rows, :])):
            wkp[p, rows, :] = x
    out_ab[...] = jnp.zeros_like(out_ab)

    load.wait()

    def biggest(i, mx):
        n, rows = where_is(i)
        x = wprime[n, rows, :]
        vprev[n, rows, :] = jnp.zeros((RB, ts), F32)
        return jnp.maximum(mx, fold(jnp.maximum, jnp.abs(x)))

    mx = lax.fori_loop(0, nblk, biggest, jnp.zeros((8, W8), F32))
    ar_start(0, two_rows(jnp.zeros((1, 128), F32), as_row(mx, jnp.max)))
    l_first.wait()
    l_split(1, per - 1, l0)
    r_first.wait()
    r_split(1, per - 1, r0)
    _, gmax = ar_wait(0)
    scaled_start(jnp.max(1.0 / vec(gmax)) * (2.0 ** -12))

    def v_copy(src, slot, s):
        return pltpu.make_async_remote_copy(
            src_ref=vy.at[src], dst_ref=vy.at[slot], send_sem=vsend.at[slot], recv_sem=vrecv.at[slot],
            device_id={"row": row_of(s)}, device_id_type=pl.DeviceIdType.MESH)

    def t1_chunk(pieces, l, keep):
        got = six([pieces[k] for k in range(3)], [vp[p] for p in range(3)])
        for n in range(4):
            at = (2 * l + n % 2, slice(None), pl.ds((n // 2) * ts, ts))
            t1[at] = jnp.where(keep, t1[at], 0.0) + got[:, n * ts:(n + 1) * ts]

    def t1_group(g, carry):
        @pl.when(g > 0)
        def _():
            v_copy(0, g, 0).wait_recv()

        @pl.when((g > 0) & (mod(g, 2) == 0))
        def _():
            v_copy(g, g + 1, 1).start()

        for n in range(4):
            for b in range(ts // SB):
                rows = pl.ds(b * SB, SB)
                for p, x in enumerate(split3(vy[g, n, rows, :])):
                    vp[p, rows, pl.ds(n * ts, ts)] = x

        def trip(hh, c2):
            @pl.when((g < 7) | (hh == 0))
            def _():
                l_batch(mod(g + hh, 8), 1 - hh, 1 - hh)

            l_batch_wait(hh)
            for k in range(per):
                l_split(hh, k, lps[pieces_of((k + 1) % per)])
                t1_chunk(lps[pieces_of(k)], per * hh + k, g > 0)
            return c2

        return lax.fori_loop(0, 2, trip, carry)

    t2_rows = min(64, hs)

    def t2_trip(factor, i, carry):
        c0 = pl.multiple_of(i * t2_rows, t2_rows)
        kron = 2 * nd * KRON
        for h in range(t2_rows // 16):
            parts = []
            for e in range(2):
                x = t1[:, pl.ds(c0 + h * 16 + e * 8, 8), :].reshape(kron, 2 * ts) * factor
                if kron < 256:
                    x = jnp.concatenate([x, jnp.zeros((256 - kron, 2 * ts), F32)], axis=0)
                got = six([wkp[k, pl.ds(0, kron), :] for k in range(3)], split3(x))
                parts.append(got.reshape(2 * nd, KRON, 2 * ts))
            for p, x in enumerate(split3(jnp.concatenate(parts, axis=1))):
                t2[p, :, pl.ds(c0 + h * 16, 16), :] = x
        return carry

    def y_copy(src, idx, slot, to):
        return pltpu.make_async_remote_copy(
            src_ref=src, dst_ref=landing(slot), send_sem=ysend.at[idx], recv_sem=yrecv.at[slot],
            device_id={"col": to}, device_id_type=pl.DeviceIdType.MESH)

    def y_ref(dm, h):
        return vy.at[4 + dm, pl.ds(2 * h, 2)]

    def landing(slot):
        return recv.at[pl.ds(2 * slot, 2)]

    def add_into(dm, h, slot):
        y_copy(landing(slot), 0, slot, col).wait_recv()

        def add(i, c):
            n, rows = where_is(i)
            vy[4 + dm, 2 * h + n, rows, :] = vy[4 + dm, 2 * h + n, rows, :] + recv[2 * slot + n, rows, :]
            return c

        lax.fori_loop(0, nblk // 2, add, 0)

    def t3_chunk(pieces, r):
        return six([t2[k, pl.ds(2 * r, 2), :, :].reshape(2 * ts, 2 * ts) for k in range(3)],
                   [pieces[k].reshape(2 * ts, ts) for k in range(3)])

    def t3_part(i, carry):
        dm, h = block_of(i)

        def trip(hh, c2):
            @pl.when((i < 7) | (hh == 0))
            def _():
                r_batch(mod(i + hh, 8), 1 - hh, 1 - hh)

            r_batch_wait(hh)
            total = None
            for k in range(per):
                r_split(hh, k, rps[pieces_of((k + 1) % per)])
                got = t3_chunk(rps[pieces_of(k)], per * hh + k)
                total = got if total is None else total + got
            yacc[...] = yacc[...] + total.reshape(2, ts, ts)
            return c2

        yacc[...] = jnp.zeros_like(yacc)
        lax.fori_loop(0, 2, trip, 0)
        vy[4 + dm, pl.ds(2 * h, 2)] = yacc[...]

        @pl.when(i == 2 * mz)
        def _():
            pl.semaphore_wait(fwd_ok, 1)

        @pl.when((mz == 1) & (i == 4))
        def _():
            pl.semaphore_wait(back_ok, 1)

        @pl.when((mz == 0) & (i < 6))
        def _():
            y_copy(y_ref(dm, h), i, i, col + zdir).start()

        @pl.when((mz == 1) & (i >= 2) & (i < 6))
        def _():
            k = i - 2
            add_into(3 - div(k, 2), mod(k, 2), k)
            y_copy(y_ref(3 - div(k, 2), mod(k, 2)), 6 + k, 6 + k, col + zdir).start()

        @pl.when((mz == 1) & (i >= 4) & (i < 6))
        def _():
            k = i - 4
            add_into(0, k, 6 + k)
            y_copy(y_ref(0, k), k, 6 + k, col - zdir).start()

        return carry

    def step(j, state):
        gmax, beta_prev = state
        for s in (1, 2, 4, 6):
            v_copy(0, s, s).start()
        lax.fori_loop(0, 8, t1_group, 0)
        for s in range(1, 8):
            v_copy(0, s, 0).wait_send()

        @pl.when(mz == 0)
        def _():
            pl.semaphore_signal(back_ok, inc=1, device_id={"col": col + zdir}, device_id_type=pl.DeviceIdType.MESH)

        @pl.when(mz == 1)
        def _():
            pl.semaphore_signal(fwd_ok, inc=1, device_id={"col": col + zdir}, device_id_type=pl.DeviceIdType.MESH)
            pl.semaphore_signal(fwd_ok, inc=1, device_id={"col": col - zdir}, device_id_type=pl.DeviceIdType.MESH)

        total, _ = ar_wait(1)
        norm_v = jnp.sqrt(vec(total))
        norm = jnp.max(norm_v)
        inv = jnp.max(1.0 / norm_v)
        factor = jnp.max(vec(gmax) / norm_v) * (2.0 ** 12)
        beta_prev = jnp.where(j > 0, norm, 0.0)
        lane = lax.broadcasted_iota(jnp.int32, (8, 128), 1)
        sub = lax.broadcasted_iota(jnp.int32, (8, 128), 0)
        out_ab[...] = jnp.where((sub == 1) & (lane == j - 1), norm_v, out_ab[...])

        lax.fori_loop(0, hs // t2_rows, functools.partial(t2_trip, factor), 0)
        r_batch(zero_i, zero_i, 0)
        lax.fori_loop(hs // t2_rows, ts // t2_rows, functools.partial(t2_trip, factor), 0)
        lax.fori_loop(0, 8, t3_part, 0)

        @pl.when(mz == 0)
        def _():
            for h in range(2):
                add_into(0, h, 6 + h)
            for k in range(6):
                y_copy(y_ref(0, 0), k, k, col).wait_send()

        @pl.when(mz == 1)
        def _():
            for h in range(2):
                add_into(1, h, 4 + h)
                add_into(1, h, 8 + h)
            for k in (0, 1, 6, 7, 8, 9):
                y_copy(y_ref(0, 0), k, k, col).wait_send()

        own = 4 + mz

        @pl.when(j < STEPS - 1)
        def _():
            l_batch(zero_i, zero_i, 0)

        def dots(i, c):
            n, rows = where_is(i)
            dot, mx = c
            w = vy[own, n, rows, :]
            v = wprime[n, rows, :] * inv
            vcur[n, rows, :] = v
            wprime[n, rows, :] = w
            return dot + fold(jnp.add, v * w), jnp.maximum(mx, fold(jnp.maximum, jnp.abs(w)))

        zero = jnp.zeros((8, W8), F32)
        dot, mx = lax.fori_loop(0, nblk, dots, (zero, zero))
        ar_start(0, two_rows(as_row(dot, jnp.sum), as_row(mx, jnp.max)))
        alpha, gmax = ar_wait(0)
        out_ab[...] = jnp.where((sub == 0) & (lane == j), vec(alpha), out_ab[...])
        small = jnp.max(1.0 / vec(gmax)) * (2.0 ** -12)

        def update(i, sq):
            n, rows = where_is(i)
            v = vcur[n, rows, :]
            x = wprime[n, rows, :] - alpha * v - beta_prev * vprev[n, rows, :]
            vprev[n, rows, :] = v
            wprime[n, rows, :] = x
            vy[0, n, rows, :] = x * small
            return sq + fold(jnp.add, x * x)

        sq = lax.fori_loop(0, nblk, update, zero)
        ar_start(1, two_rows(as_row(sq, jnp.sum), jnp.zeros((1, 128), F32)))
        return gmax, norm

    lax.fori_loop(0, STEPS, step, (gmax, jnp.float32(0)))

    total, _ = ar_wait(1)
    norm_v = jnp.sqrt(vec(total))
    inv = jnp.max(1.0 / norm_v)
    lane = lax.broadcasted_iota(jnp.int32, (8, 128), 1)
    sub = lax.broadcasted_iota(jnp.int32, (8, 128), 0)
    out_ab[...] = jnp.where((sub == 1) & (lane == STEPS - 1), norm_v, out_ab[...])

    def last(i, c):
        n, rows = where_is(i)
        wprime[n, rows, :] = wprime[n, rows, :] * inv
        return c

    lax.fori_loop(0, nblk, last, 0)
    store = pltpu.make_async_copy(wprime, out_v, iosem)
    store.start()
    store.wait()


def local_steps(ts, nd, psi_blk, left_blk, mpo_tensor, right_blk):
    psi = psi_blk.reshape(ts, 2, 2, ts).transpose(2, 1, 0, 3).reshape(4, ts, ts)
    lt = left_blk.transpose(1, 0, 2)
    rt = right_blk.transpose(1, 0, 2).reshape(4 * nd, ts // 2, 8 * ts)
    w2 = mpo_tensor.transpose(1, 3, 0, 2).reshape(2 * nd, 1, 2 * nd, 1)
    eye = jnp.eye(KRON, dtype=F32).reshape(1, KRON, 1, KRON)
    wk = (w2 * eye).reshape(2 * nd * KRON, 2 * nd * KRON)
    pad = 256 - 2 * nd * KRON
    wk = jnp.pad(wk, ((0, pad), (0, pad)))
    any_space = pl.BlockSpec(memory_space=pl.ANY)
    vmem = pl.BlockSpec(memory_space=pltpu.VMEM)
    dma, V = pltpu.SemaphoreType.DMA, pltpu.VMEM
    out_v, out_ab = pl.pallas_call(
        functools.partial(lanczos_kernel, ts, nd),
        out_shape=(jax.ShapeDtypeStruct((4, ts, ts), F32), jax.ShapeDtypeStruct((8, 128), F32)),
        in_specs=[any_space, vmem, any_space, any_space],
        out_specs=(any_space, vmem),
        scratch_shapes=[
            V((8, 4, ts, ts), F32), V((4, ts, ts), F32), V((4, ts, ts), F32), V((4, ts, ts), F32),
            V((20, ts, ts), F32), V((2 * nd, ts, 2 * ts), F32), V((3, 2 * nd, ts, 2 * ts), BF16),
            V((3, ts, ts), BF16), V((3, ts, ts), BF16), V((3, ts, ts), BF16),
            V((3, 2, ts, ts), BF16), V((3, 2, ts, ts), BF16), V((3, 2, ts, ts), BF16),
            V((3, ts, 4 * ts), BF16), V((3, 256, 256), BF16), V((2, ts, ts), F32),
            V((2, 2, 128), F32), V((2, NDEV, 2, 128), F32),
            dma((2,)), dma((2,)), dma((8,)), dma((8,)), dma((10,)), dma((10,)), dma((2,)), dma((2,)), dma,
            pltpu.SemaphoreType.REGULAR, pltpu.SemaphoreType.REGULAR,
        ],
        compiler_params=pltpu.CompilerParams(vmem_limit_bytes=67043328, has_side_effects=True),
    )(psi, wk, lt, rt)
    v_next = out_v.reshape(2, 2, ts, ts).transpose(2, 1, 0, 3).reshape(ts, 2, 2 * ts)
    return out_ab[0, :STEPS], out_ab[1, :STEPS], v_next


def build(mesh, ts, nd):
    return jax.shard_map(
        functools.partial(local_steps, ts, nd), mesh=mesh,
        in_specs=(P("row", None, "col"), P("row", None, None), P(), P("col", None, None)),
        out_specs=(P(), P(), P("row", None, "col")), check_vma=False)


def solution(mesh):
    return build(mesh, 256, 14)
```

```python
import functools

import jax
import jax.numpy as jnp
from jax import lax
from jax.experimental import pallas as pl
from jax.experimental.pallas import tpu as pltpu
from jax.sharding import PartitionSpec as P

F32, BF16 = jnp.float32, jnp.bfloat16
STEPS = 4
NROW, NCOL = 8, 4
NDEV = NROW * NCOL
KRON = 4
PASSES = ((0, 3), (1, 2), (2, 1))


def div(a, b):
    return lax.div(a, jnp.int32(b))


def mod(a, b):
    return lax.rem(a, jnp.int32(b))


def split3(x):
    hi = x.astype(BF16)
    rest = x - hi.astype(F32)
    mid = rest.astype(BF16)
    low = (rest - mid.astype(F32)).astype(BF16)
    return hi, mid, low


def lanczos_kernel(ts, nd, psi, w2, lt, rt, out_v, out_a, out_b,
                   psi_v, vy, vcur, vprev, wprime, recv, t1, t2, l0, l1, r0, r1, vp, wk6, ar_src, ar_recv,
                   lsem, rsem, vsend, vrecv, ysend, yrecv, asend, arecv, iosem, fwd_ok, back_ok):
    row, col = lax.axis_index("row"), lax.axis_index("col")
    me = col * NROW + row
    core, xx, yy = mod(row, 2), mod(div(row, 2), 2), div(row, 4)
    hs = ts // 2
    kron = 2 * nd * KRON
    lps, rps = (l0, l1), (r0, r1)

    def six(lhs, rhs):
        a = [x for p, n in PASSES for x in lhs[:n]]
        b = [rhs[p] for p, n in PASSES for _ in range(n)]
        return jnp.dot(jnp.concatenate(a, axis=1), jnp.concatenate(b, axis=0), preferred_element_type=F32)

    def row_of(s):
        hi, two, odd = div(s, 4), mod(div(s, 2), 2), mod(s, 2)
        fp = (1 - hi) * two * (1 - odd) + hi * (two + (1 - two) * odd)
        fq = (1 - hi) * two * odd + hi * (two + (1 - two) * (1 - odd))
        fx, fy = (1 - core) * fp + core * fq, (1 - core) * fq + core * fp
        c2, x2, y2 = core + odd - 2 * core * odd, xx + fx - 2 * xx * fx, yy + fy - 2 * yy * fy
        return (y2 * 2 + x2) * 2 + c2

    half_z = div(col, 2)
    zdir = 1 - 2 * half_z
    mz = col + half_z * (3 - 2 * col)

    def block_of(i):
        late, two, odd = div(i, 4), div(i, 2), mod(i, 2)
        d_in = (1 - late) * 3 * (1 - odd) + late * (4 - two)
        h_in = (1 - late) * two + late * odd
        return (1 - mz) * (3 - two) + mz * d_in, (1 - mz) * odd + mz * h_in

    def l_batch(g):
        slot = mod(g, 2)
        a0 = pl.multiple_of(row_of(g) * ts, ts)
        a1 = pl.multiple_of(row_of(mod(g + 1, 8)) * ts, ts)
        pltpu.make_async_copy(lt.at[pl.ds(1, nd - 1), :, pl.ds(a0, ts)],
                              recv.at[pl.ds(nd * slot, nd - 1)], lsem.at[slot]).start()
        pltpu.make_async_copy(lt.at[pl.ds(0, 1), :, pl.ds(a1, ts)],
                              recv.at[pl.ds(nd * slot + nd - 1, 1)], lsem.at[slot]).start()

    def l_batch_wait(slot):
        ref = recv.at[pl.ds(nd * slot, nd)]
        pltpu.make_async_copy(ref, ref, lsem.at[slot]).wait()

    def r_start(i):
        dm, h = block_of(i)
        dest = dm + half_z * (3 - 2 * dm)
        return pl.multiple_of((dest * 2 + h) * ts, ts)

    def r_rows(slot):
        return pl.ds(pl.multiple_of(slot * hs, hs), hs)

    half = nd // 2

    def r_batch(i):
        slot = mod(i, 2)
        d0, d1 = r_start(i), r_start(mod(i + 1, 8))
        for first, count, d, hh, plane in ((1, half, d0, 0, 0), (half + 1, half - 1, d0, 1, 0), (0, 1, d1, 1, 4 * half - 4)):
            if count:
                pltpu.make_async_copy(rt.at[pl.ds(4 * first, 4 * count), :, pl.ds(d, ts)],
                                      t1.at[pl.ds(plane, 4 * count), r_rows(slot), pl.ds(hh * ts, ts)],
                                      rsem.at[slot]).start()

    def r_batch_wait(slot):
        ref = t1.at[pl.ds(0, 4 * half), r_rows(slot)]
        pltpu.make_async_copy(ref, ref, rsem.at[slot]).wait()

    SB = min(32, ts)

    def l_split(slot, k, dst):
        for b in range(ts // SB):
            rows = pl.ds(b * SB, SB)
            for p, x in enumerate(split3(recv[nd * slot + k, rows, :])):
                dst[p, rows, :] = x

    def r_split(slot, k, dst):
        hh, kk = k // half, k % half
        sb = min(SB, hs)
        for kb in range(2):
            for bh in range(2):
                for b in range(hs // sb):
                    rows = pl.ds(pl.multiple_of(slot * hs + b * sb, sb), sb)
                    for p, x in enumerate(split3(t1[4 * kk + 2 * kb + bh, rows, pl.ds(hh * ts, ts)])):
                        dst[p, kb, pl.ds(bh * hs + b * sb, sb), :] = x

    def ar_start(slot, tile):
        ar_src[slot] = tile
        ar_recv[slot, me] = tile

        def send(off, carry):
            to = mod(me + off, NDEV)
            pltpu.make_async_remote_copy(
                src_ref=ar_src.at[slot], dst_ref=ar_recv.at[slot, me], send_sem=asend.at[slot], recv_sem=arecv.at[slot],
                device_id={"col": div(to, NROW), "row": mod(to, NROW)}, device_id_type=pl.DeviceIdType.MESH).start()
            return carry

        lax.fori_loop(1, NDEV, send, 0)

    def ar_wait(slot):
        every = ar_recv.at[slot, pl.ds(0, NDEV - 1)]
        copy = pltpu.make_async_remote_copy(
            src_ref=every, dst_ref=every, send_sem=asend.at[slot], recv_sem=arecv.at[slot],
            device_id={"col": col, "row": row}, device_id_type=pl.DeviceIdType.MESH)
        copy.wait_send()
        copy.wait_recv()
        got = ar_recv[slot]
        first = lax.broadcasted_iota(jnp.int32, got.shape, 1) == 0
        return jnp.sum(jnp.where(first, got, 0.0)), jnp.max(jnp.where(first, 0.0, got))

    RB = min(64, ts)
    nblk = 4 * (ts // RB)

    def where_is(i):
        return div(i, ts // RB), pl.ds(pl.multiple_of(mod(i, ts // RB) * RB, RB), RB)

    def fold(op, x):
        x = x.reshape(RB // 8, 8, ts)
        y = x[0]
        for k in range(1, RB // 8):
            y = op(y, x[k])
        if ts <= 128:
            return y
        return op(y[:, :128], y[:, 128:])

    W8 = min(128, ts)

    def as_row(x, op):
        x = op(x, axis=0, keepdims=True)
        return x if W8 == 128 else jnp.concatenate([x, jnp.zeros((1, 128 - W8), F32)], axis=1)

    def two_rows(a, b):
        first = lax.broadcasted_iota(jnp.int32, (2, 128), 0) == 0
        return jnp.where(first, jnp.broadcast_to(a, (2, 128)), jnp.broadcast_to(b, (2, 128)))

    def vec(x):
        return jnp.full((8, 128), x, F32)

    def scaled_start(src_norm_coef):
        def scale(i, sq):
            n, rows = where_is(i)
            x = wprime[n, rows, :]
            vy[0, n, rows, :] = x * src_norm_coef
            return sq + fold(jnp.add, x * x)

        sq = lax.fori_loop(0, nblk, scale, jnp.zeros((8, W8), F32))
        ar_start(1, two_rows(as_row(sq, jnp.sum), jnp.zeros((1, 128), F32)))

    LB = min(128, ts)
    blocks = range(2 * ts // LB)
    loads = [pltpu.make_async_copy(psi.at[:, pl.ds(b * LB, LB)], psi_v.at[b], iosem.at[b]) for b in blocks]
    for load in loads:
        load.start()
    l_first = pltpu.make_async_copy(lt.at[pl.ds(0, 1), :, pl.ds(pl.multiple_of(row * ts, ts), ts)],
                                    recv.at[pl.ds(2 * nd - 1, 1)], lsem.at[1])
    l_first.start()
    zero_i = jnp.int32(0)
    r_first = pltpu.make_async_copy(rt.at[pl.ds(0, 4), :, pl.ds(r_start(zero_i), ts)],
                                    t1.at[pl.ds(4 * half - 4, 4), r_rows(1), pl.ds(ts, ts)], rsem.at[1])
    r_first.start()
    l_batch(zero_i)
    for b, load in enumerate(loads):
        load.wait()
        for sp in range(2):
            wprime[2 * (b * LB // ts) + sp, :, pl.ds(b * LB % ts, LB)] = psi_v[b, pl.ds(sp, ts, stride=2), :]

    def biggest(i, mx):
        n, rows = where_is(i)
        x = wprime[n, rows, :]
        vprev[n, rows, :] = jnp.zeros((RB, ts), F32)
        return jnp.maximum(mx, fold(jnp.maximum, jnp.abs(x)))

    mx = lax.fori_loop(0, nblk, biggest, jnp.zeros((8, W8), F32))
    ar_start(0, two_rows(jnp.zeros((1, 128), F32), as_row(mx, jnp.max)))
    pieces = split3(w2[...])
    up = (div(lax.broadcasted_iota(jnp.int32, (kron, 2 * nd), 0), KRON)
          == lax.broadcasted_iota(jnp.int32, (kron, 2 * nd), 1)).astype(F32).astype(BF16)
    lane = lax.broadcasted_iota(jnp.int32, (2 * nd, 6 * kron), 1)
    across = (div(mod(lane, kron), KRON) == lax.broadcasted_iota(jnp.int32, (2 * nd, 6 * kron), 0)).astype(F32).astype(BF16)
    lane = lax.broadcasted_iota(jnp.int32, (kron, 6 * kron), 1)
    same = mod(lane, KRON) == mod(lax.broadcasted_iota(jnp.int32, (kron, 6 * kron), 0), KRON)
    which = div(lane, kron)
    total = jnp.zeros((kron, 6 * kron), F32)
    for k in range(3):
        tall = jnp.dot(up, pieces[k], preferred_element_type=F32).astype(BF16)
        wide = jnp.dot(tall, across, preferred_element_type=F32)
        here = [n for n, kk in enumerate(kk for p, n2 in PASSES for kk in range(n2)) if kk == k]
        mask = same & functools.reduce(jnp.logical_or, [which == n for n in here])
        total = jnp.where(mask, wide, total)
    wk6[...] = total.astype(BF16)
    l_first.wait()
    l_split(1, nd - 1, l0)
    r_first.wait()
    r_split(1, nd - 1, r0)
    _, gmax = ar_wait(0)
    scaled_start(jnp.max(1.0 / vec(gmax)) * (2.0 ** -12))

    def v_copy(src, slot, s):
        return pltpu.make_async_remote_copy(
            src_ref=vy.at[src], dst_ref=vy.at[slot], send_sem=vsend.at[slot], recv_sem=vrecv.at[slot],
            device_id={"row": row_of(s)}, device_id_type=pl.DeviceIdType.MESH)

    def swap(a, b):
        a, b = a.reshape(-1, 8, a.shape[-1]), b.reshape(-1, 8, b.shape[-1])
        low = lax.broadcasted_iota(jnp.int32, a.shape, 1) < 4
        return jnp.where(low, a, pltpu.roll(b, 4, 1)), jnp.where(low, pltpu.roll(a, 4, 1), b)

    def t1_chunk(pieces, l, keep):
        got = six([pieces[k] for k in range(3)], [vp[p] for p in range(3)])
        for bh in range(2):
            both = swap(got[:, 2 * bh * ts:(2 * bh + 1) * ts], got[:, (2 * bh + 1) * ts:(2 * bh + 2) * ts])
            for e in range(2):
                at = (2 * l + e, slice(None), pl.ds(bh * ts, ts))
                t1[at] = jnp.where(keep, t1[at], 0.0) + both[e].reshape(ts, ts)

    def t1_group(g, carry):
        @pl.when(g > 0)
        def _():
            v_copy(0, g, 0).wait_recv()

        @pl.when((g > 0) & (mod(g, 2) == 0))
        def _():
            v_copy(g, g + 1, 1).start()

        @pl.when((g == 1) | (g == 2))
        def _():
            v_copy(0, 2 + 2 * g, 2 + 2 * g).start()

        @pl.when(g < 7)
        def _():
            l_batch(g + 1)

        slot = mod(g, 2)
        l_batch_wait(slot)
        for n in range(4):
            for b in range(ts // SB):
                rows = pl.ds(b * SB, SB)
                for p, x in enumerate(split3(vy[g, n, rows, :])):
                    vp[p, rows, pl.ds(n * ts, ts)] = x
        for k in range(nd):
            l_split(slot, k, lps[(k + 1) % 2])
            t1_chunk(lps[k % 2], k, g > 0)
        return carry

    t2_rows = min(64, hs)

    def t2_trip(i, carry):
        @pl.when(i == (hs // t2_rows))
        def _():
            r_batch(zero_i)

        c0 = pl.multiple_of(i * t2_rows, t2_rows)
        for h in range(t2_rows // 8):
            x = t1[:, pl.ds(c0 + h * 8, 8), :].reshape(nd, 2, 8, 2 * ts)
            parts = []
            for e in range(2):
                b = split3(x[:, e].reshape(kron, 2 * ts))
                rhs = jnp.concatenate([b[p] for p, n in PASSES for _ in range(n)], axis=0)
                got = jnp.dot(wk6[...], rhs, preferred_element_type=F32)
                parts.append(got.reshape(nd, 8, 2 * ts))
            for p, y in enumerate(split3(jnp.concatenate(parts, axis=1))):
                t2[p, :, pl.ds(2 * c0 + h * 16, 16), :] = y
        return carry

    def y_copy(src, idx, slot, to):
        return pltpu.make_async_remote_copy(
            src_ref=src, dst_ref=landing(slot), send_sem=ysend.at[idx], recv_sem=yrecv.at[slot],
            device_id={"col": to}, device_id_type=pl.DeviceIdType.MESH)

    def y_ref(dm, h):
        return vy.at[4 + dm, pl.ds(2 * h, 2)]

    def landing(slot):
        return recv.at[pl.ds(2 * slot, 2)]

    def add_into(dm, h, slot):
        y_copy(landing(slot), 0, slot, col).wait_recv()

        def add(i, c):
            n, rows = where_is(i)
            vy[4 + dm, 2 * h + n, rows, :] = vy[4 + dm, 2 * h + n, rows, :] + recv[2 * slot + n, rows, :]
            return c

        lax.fori_loop(0, nblk // 2, add, 0)

    def t3_chunk(pieces, r):
        return six([t2[k, r] for k in range(3)],
                   [pieces[k].reshape(2 * ts, ts) for k in range(3)])

    def t3_part(factor, i, carry):
        dm, h = block_of(i)

        @pl.when(i < 7)
        def _():
            r_batch(i + 1)

        slot = mod(i, 2)
        r_batch_wait(slot)
        total = None
        for k in range(nd):
            r_split(slot, k, rps[(k + 1) % 2])
            got = t3_chunk(rps[k % 2], k)
            total = got if total is None else total + got
        total = (total * factor).reshape(ts // 8, 16, ts)
        for e, y in enumerate(swap(total[:, :8], total[:, 8:])):
            vy[4 + dm, 2 * h + e] = y.reshape(ts, ts)

        @pl.when(i == 2 * mz)
        def _():
            pl.semaphore_wait(fwd_ok, 1)

        @pl.when((mz == 1) & (i == 4))
        def _():
            pl.semaphore_wait(back_ok, 1)

        @pl.when((mz == 0) & (i < 6))
        def _():
            y_copy(y_ref(dm, h), i, i, col + zdir).start()

        @pl.when((mz == 1) & (i >= 2) & (i < 6))
        def _():
            k = i - 2
            add_into(3 - div(k, 2), mod(k, 2), k)
            y_copy(y_ref(3 - div(k, 2), mod(k, 2)), 6 + k, 6 + k, col + zdir).start()

        @pl.when((mz == 1) & (i >= 4) & (i < 6))
        def _():
            k = i - 4
            add_into(0, k, 6 + k)
            y_copy(y_ref(0, k), k, 6 + k, col - zdir).start()

        return carry

    def step(j, state):
        gmax, beta_prev = state
        for s in (1, 2):
            v_copy(0, s, s).start()
        lax.fori_loop(0, 8, t1_group, 0)
        for s in range(1, 8):
            v_copy(0, s, 0).wait_send()

        @pl.when(mz == 0)
        def _():
            pl.semaphore_signal(back_ok, inc=1, device_id={"col": col + zdir}, device_id_type=pl.DeviceIdType.MESH)

        @pl.when(mz == 1)
        def _():
            pl.semaphore_signal(fwd_ok, inc=1, device_id={"col": col + zdir}, device_id_type=pl.DeviceIdType.MESH)
            pl.semaphore_signal(fwd_ok, inc=1, device_id={"col": col - zdir}, device_id_type=pl.DeviceIdType.MESH)

        total, _ = ar_wait(1)
        norm_v = jnp.sqrt(vec(total))
        norm = jnp.max(norm_v)
        inv = jnp.max(1.0 / norm_v)
        factor = jnp.max(vec(gmax) / norm_v) * (2.0 ** 12)
        beta_prev = jnp.where(j > 0, norm, 0.0)

        @pl.when(j > 0)
        def _():
            out_b[j - 1] = norm

        lax.fori_loop(0, ts // t2_rows, t2_trip, 0)
        lax.fori_loop(0, 8, functools.partial(t3_part, factor), 0)

        @pl.when(mz == 0)
        def _():
            for h in range(2):
                add_into(0, h, 6 + h)
            for k in range(6):
                y_copy(y_ref(0, 0), k, k, col).wait_send()

        @pl.when(mz == 1)
        def _():
            for h in range(2):
                add_into(1, h, 4 + h)
                add_into(1, h, 8 + h)
            for k in (0, 1, 6, 7, 8, 9):
                y_copy(y_ref(0, 0), k, k, col).wait_send()

        own = 4 + mz

        @pl.when(j < STEPS - 1)
        def _():
            l_batch(zero_i)

        def dots(i, c):
            n, rows = where_is(i)
            dot, mx = c
            w = vy[own, n, rows, :]
            v = wprime[n, rows, :] * inv
            vcur[n, rows, :] = v
            wprime[n, rows, :] = w
            return dot + fold(jnp.add, v * w), jnp.maximum(mx, fold(jnp.maximum, jnp.abs(w)))

        zero = jnp.zeros((8, W8), F32)
        dot, mx = lax.fori_loop(0, nblk, dots, (zero, zero))
        ar_start(0, two_rows(as_row(dot, jnp.sum), as_row(mx, jnp.max)))
        alpha, gmax = ar_wait(0)
        out_a[j] = alpha
        small = jnp.max(1.0 / vec(gmax)) * (2.0 ** -12)

        def update(i, sq):
            n, rows = where_is(i)
            v = vcur[n, rows, :]
            x = wprime[n, rows, :] - alpha * v - beta_prev * vprev[n, rows, :]
            vprev[n, rows, :] = v
            wprime[n, rows, :] = x
            vy[0, n, rows, :] = x * small
            return sq + fold(jnp.add, x * x)

        sq = lax.fori_loop(0, nblk, update, zero)
        ar_start(1, two_rows(as_row(sq, jnp.sum), jnp.zeros((1, 128), F32)))
        return gmax, norm

    lax.fori_loop(0, STEPS, step, (gmax, jnp.float32(0)))

    total, _ = ar_wait(1)
    norm_v = jnp.sqrt(vec(total))
    inv = jnp.max(1.0 / norm_v)
    out_b[STEPS - 1] = jnp.max(norm_v)

    stores = [pltpu.make_async_copy(psi_v.at[b], out_v.at[:, pl.ds(b * LB, LB)], iosem.at[b]) for b in blocks]
    for b, store in enumerate(stores):
        for sp in range(2):
            psi_v[b, pl.ds(sp, ts, stride=2), :] = wprime[2 * (b * LB // ts) + sp, :, pl.ds(b * LB % ts, LB)] * inv
        store.start()
    for store in stores:
        store.wait()


def local_steps(ts, nd, psi_blk, left_blk, mpo_tensor, right_blk):
    psi = psi_blk.reshape(2 * ts, 2 * ts)
    lt = left_blk.transpose(1, 0, 2)
    rt = right_blk.transpose(1, 0, 2).reshape(4 * nd, ts // 2, 8 * ts)
    w2 = mpo_tensor.transpose(1, 3, 0, 2).reshape(2 * nd, 2 * nd)
    any_space = pl.BlockSpec(memory_space=pl.ANY)
    vmem = pl.BlockSpec(memory_space=pltpu.VMEM)
    dma, V = pltpu.SemaphoreType.DMA, pltpu.VMEM
    smem = pl.BlockSpec(memory_space=pltpu.SMEM)
    out_v, alpha, beta = pl.pallas_call(
        functools.partial(lanczos_kernel, ts, nd),
        out_shape=(jax.ShapeDtypeStruct((2 * ts, 2 * ts), F32),) + (jax.ShapeDtypeStruct((STEPS,), F32),) * 2,
        in_specs=[any_space, vmem, any_space, any_space],
        out_specs=(any_space, smem, smem),
        scratch_shapes=[
            V((2 * ts // min(128, ts), 2 * ts, min(128, ts)), F32), V((8, 4, ts, ts), F32), V((4, ts, ts), F32), V((4, ts, ts), F32), V((4, ts, ts), F32),
            V((max(20, 2 * nd), ts, ts), F32), V((2 * nd, ts, 2 * ts), F32), V((3, nd, 2 * ts, 2 * ts), BF16),
            V((3, ts, ts), BF16), V((3, ts, ts), BF16), V((3, 2, ts, ts), BF16), V((3, 2, ts, ts), BF16),
            V((3, ts, 4 * ts), BF16), V((2 * nd * KRON, 12 * nd * KRON), BF16),
            V((2, 2, 128), F32), V((2, NDEV, 2, 128), F32),
            dma((2,)), dma((2,)), dma((8,)), dma((8,)), dma((10,)), dma((10,)), dma((2,)), dma((2,)), dma((4,)),
            pltpu.SemaphoreType.REGULAR, pltpu.SemaphoreType.REGULAR,
        ],
        compiler_params=pltpu.CompilerParams(vmem_limit_bytes=67043328, has_side_effects=True),
    )(psi, w2, lt, rt)
    return alpha, beta, out_v.reshape(ts, 2, 2 * ts)


def build(mesh, ts, nd):
    return jax.shard_map(
        functools.partial(local_steps, ts, nd), mesh=mesh,
        in_specs=(P("row", None, "col"), P("row", None, None), P(), P("col", None, None)),
        out_specs=(P(), P(), P("row", None, "col")), check_vma=False)


def solution(mesh):
    return build(mesh, 256, 14)
```

```python
import functools

import jax
import jax.numpy as jnp
from jax import lax
from jax.experimental import pallas as pl
from jax.experimental.pallas import tpu as pltpu
from jax.sharding import PartitionSpec as P

F32, BF16 = jnp.float32, jnp.bfloat16
STEPS = 4
NROW, NCOL = 8, 4
NDEV = NROW * NCOL
KRON = 4
PASSES = ((0, 3), (1, 2), (2, 1))


def div(a, b):
    return lax.div(a, jnp.int32(b))


def mod(a, b):
    return lax.rem(a, jnp.int32(b))


def split3(x):
    hi = x.astype(BF16)
    rest = x - hi.astype(F32)
    mid = rest.astype(BF16)
    low = (rest - mid.astype(F32)).astype(BF16)
    return hi, mid, low


def lanczos_kernel(ts, nd, psi, w_in, lt, rt, out_v, out_ab,
                   psi_v, wv, norms, vy, vcur, vprev, wprime, recv, t1, t2, l0, l1, r0, r1, vp, wk6, ar_src, ar_recv,
                   lsem, rsem, vsend, vrecv, ysend, yrecv, asend, arecv, iosem, wsem, fwd_ok, back_ok):
    row, col = lax.axis_index("row"), lax.axis_index("col")
    me = col * NROW + row
    core, xx, yy = mod(row, 2), mod(div(row, 2), 2), div(row, 4)
    hs = ts // 2
    kron = 2 * nd * KRON
    lps, rps = (l0, l1), (r0, r1)

    def six(lhs, rhs):
        a = [x for p, n in PASSES for x in lhs[:n]]
        b = [rhs[p] for p, n in PASSES for _ in range(n)]
        return jnp.dot(jnp.concatenate(a, axis=1), jnp.concatenate(b, axis=0), preferred_element_type=F32)

    def row_of(s):
        hi, two, odd = div(s, 4), mod(div(s, 2), 2), mod(s, 2)
        fp = (1 - hi) * two * (1 - odd) + hi * (two + (1 - two) * odd)
        fq = (1 - hi) * two * odd + hi * (two + (1 - two) * (1 - odd))
        fx, fy = (1 - core) * fp + core * fq, (1 - core) * fq + core * fp
        c2, x2, y2 = core + odd - 2 * core * odd, xx + fx - 2 * xx * fx, yy + fy - 2 * yy * fy
        return (y2 * 2 + x2) * 2 + c2

    half_z = div(col, 2)
    zdir = 1 - 2 * half_z
    mz = col + half_z * (3 - 2 * col)

    def block_of(i):
        late, two, odd = div(i, 4), div(i, 2), mod(i, 2)
        d_in = (1 - late) * 3 * (1 - odd) + late * (4 - two)
        h_in = (1 - late) * two + late * odd
        return (1 - mz) * (3 - two) + mz * d_in, (1 - mz) * odd + mz * h_in

    def l_start(g):
        return pl.multiple_of(row_of(mod(g, 8)) * ts, ts)

    def l_batch(slot, a0, a1):
        pltpu.make_async_copy(lt.at[pl.ds(1, nd - 1), :, pl.ds(pl.multiple_of(a0, ts), ts)],
                              recv.at[pl.ds(nd * slot, nd - 1)], lsem.at[slot]).start()
        pltpu.make_async_copy(lt.at[pl.ds(0, 1), :, pl.ds(pl.multiple_of(a1, ts), ts)],
                              recv.at[pl.ds(nd * slot + nd - 1, 1)], lsem.at[slot]).start()

    def l_batch_wait(slot):
        ref = recv.at[pl.ds(nd * slot, nd)]
        pltpu.make_async_copy(ref, ref, lsem.at[slot]).wait()

    def r_start(i):
        dm, h = block_of(mod(i, 8))
        dest = dm + half_z * (3 - 2 * dm)
        return pl.multiple_of((dest * 2 + h) * ts, ts)

    def r_rows(slot):
        return pl.ds(pl.multiple_of(slot * hs, hs), hs)

    half = nd // 2

    def r_batch(slot, d0, d1):
        for first, count, d, hh, plane in ((1, half, d0, 0, 0), (half + 1, half - 1, d0, 1, 0), (0, 1, d1, 1, 4 * half - 4)):
            if count:
                pltpu.make_async_copy(rt.at[pl.ds(4 * first, 4 * count), :, pl.ds(pl.multiple_of(d, ts), ts)],
                                      t1.at[pl.ds(plane, 4 * count), r_rows(slot), pl.ds(hh * ts, ts)],
                                      rsem.at[slot]).start()

    def r_batch_wait(slot):
        ref = t1.at[pl.ds(0, 4 * half), r_rows(slot)]
        pltpu.make_async_copy(ref, ref, rsem.at[slot]).wait()

    SB = min(32, ts)

    def l_split(slot, k, dst):
        for b in range(ts // SB):
            rows = pl.ds(b * SB, SB)
            for p, x in enumerate(split3(recv[nd * slot + k, rows, :])):
                dst[p, rows, :] = x

    def r_split(slot, k, dst):
        hh, kk = k // half, k % half
        sb = min(SB, hs)
        for kb in range(2):
            for bh in range(2):
                for b in range(hs // sb):
                    rows = pl.ds(pl.multiple_of(slot * hs + b * sb, sb), sb)
                    for p, x in enumerate(split3(t1[4 * kk + 2 * kb + bh, rows, pl.ds(hh * ts, ts)])):
                        dst[p, kb, pl.ds(bh * hs + b * sb, sb), :] = x

    def ar_start(slot, tile):
        ar_src[slot] = tile
        ar_recv[slot, me] = tile

        def send(off, carry):
            to = mod(me + off, NDEV)
            pltpu.make_async_remote_copy(
                src_ref=ar_src.at[slot], dst_ref=ar_recv.at[slot, me], send_sem=asend.at[slot], recv_sem=arecv.at[slot],
                device_id={"col": div(to, NROW), "row": mod(to, NROW)}, device_id_type=pl.DeviceIdType.MESH).start()
            return carry

        lax.fori_loop(1, NDEV, send, 0)

    def ar_wait(slot):
        every = ar_recv.at[slot, pl.ds(0, NDEV - 1)]
        copy = pltpu.make_async_remote_copy(
            src_ref=every, dst_ref=every, send_sem=asend.at[slot], recv_sem=arecv.at[slot],
            device_id={"col": col, "row": row}, device_id_type=pl.DeviceIdType.MESH)
        copy.wait_send()
        copy.wait_recv()
        got = ar_recv[slot]
        first = lax.broadcasted_iota(jnp.int32, got.shape, 1) == 0
        return jnp.sum(jnp.where(first, got, 0.0)), jnp.max(jnp.where(first, 0.0, got))

    RB = min(64, ts)
    nblk = 4 * (ts // RB)

    def where_is(i):
        return div(i, ts // RB), pl.ds(pl.multiple_of(mod(i, ts // RB) * RB, RB), RB)

    def fold(op, x):
        x = x.reshape(RB // 8, 8, ts)
        y = x[0]
        for k in range(1, RB // 8):
            y = op(y, x[k])
        if ts <= 128:
            return y
        return op(y[:, :128], y[:, 128:])

    W8 = min(128, ts)

    def as_row(x, op):
        x = op(x, axis=0, keepdims=True)
        return x if W8 == 128 else jnp.concatenate([x, jnp.zeros((1, 128 - W8), F32)], axis=1)

    def two_rows(a, b):
        first = lax.broadcasted_iota(jnp.int32, (2, 128), 0) == 0
        return jnp.where(first, jnp.broadcast_to(a, (2, 128)), jnp.broadcast_to(b, (2, 128)))

    def vec(x):
        return jnp.full((8, W8), x, F32)

    def times(x, v):
        wide = v if x.shape[-1] == v.shape[-1] else jnp.concatenate([v] * (x.shape[-1] // v.shape[-1]), axis=1)
        return (x.reshape(-1, 8, x.shape[-1]) * wide[None]).reshape(x.shape)

    def first_start(scale):
        def part(i, sq):
            n, rows = where_is(i)
            x = wprime[n, rows, :]
            vy[0, n, rows, :] = times(x, scale)
            return sq + fold(jnp.add, x * x)

        sq = lax.fori_loop(0, nblk, part, jnp.zeros((8, W8), F32))
        ar_start(1, two_rows(as_row(sq, jnp.sum), jnp.zeros((1, 128), F32)))

    barrier = pltpu.get_barrier_semaphore()

    def arrive(off, carry):
        to = mod(me + off, NDEV)
        pl.semaphore_signal(barrier, inc=1, device_id={"col": div(to, NROW), "row": mod(to, NROW)},
                            device_id_type=pl.DeviceIdType.MESH)
        return carry

    lax.fori_loop(1, NDEV, arrive, 0)
    LB = min(128, ts)
    blocks = range(2 * ts // LB)
    loads = [pltpu.make_async_copy(psi.at[:, :, pl.ds(b * LB, LB)], psi_v.at[b].reshape(ts, 2, LB), iosem.at[b]) for b in blocks]
    for load in loads:
        load.start()
    w_load = pltpu.make_async_copy(w_in, wv, wsem)
    w_load.start()
    l_first = pltpu.make_async_copy(lt.at[pl.ds(0, 1), :, pl.ds(pl.multiple_of(row * ts, ts), ts)],
                                    recv.at[pl.ds(2 * nd - 1, 1)], lsem.at[1])
    l_first.start()
    zero_i = jnp.int32(0)
    r_first = pltpu.make_async_copy(rt.at[pl.ds(0, 4), :, pl.ds(r_start(zero_i), ts)],
                                    t1.at[pl.ds(4 * half - 4, 4), r_rows(1), pl.ds(ts, ts)], rsem.at[1])
    r_first.start()
    l_batch(zero_i, l_start(zero_i), l_start(zero_i + 1))
    for b, load in enumerate(loads):
        load.wait()
        for sp in range(2):
            wprime[2 * (b * LB // ts) + sp, :, pl.ds(b * LB % ts, LB)] = psi_v[b, pl.ds(sp, ts, stride=2), :]

    def biggest(i, mx):
        n, rows = where_is(i)
        x = wprime[n, rows, :]
        vprev[n, rows, :] = jnp.zeros((RB, ts), F32)
        return jnp.maximum(mx, fold(jnp.maximum, jnp.abs(x)))

    mx = lax.fori_loop(0, nblk, biggest, jnp.zeros((8, W8), F32))
    pl.semaphore_wait(barrier, NDEV - 1)
    ar_start(0, two_rows(jnp.zeros((1, 128), F32), as_row(mx, jnp.max)))
    w_load.wait()
    pieces = [split3(wv[:, t, :]) for t in range(2)]
    at_row = lax.broadcasted_iota(jnp.int32, (kron, nd), 0)
    up = [((div(at_row, 2 * KRON) == lax.broadcasted_iota(jnp.int32, (kron, nd), 1)) & (mod(div(at_row, KRON), 2) == t))
          .astype(F32).astype(BF16) for t in range(2)]
    lane = lax.broadcasted_iota(jnp.int32, (2 * nd, 6 * kron), 1)
    across = (div(mod(lane, kron), KRON) == lax.broadcasted_iota(jnp.int32, (2 * nd, 6 * kron), 0)).astype(F32).astype(BF16)
    lane = lax.broadcasted_iota(jnp.int32, (kron, 6 * kron), 1)
    same = mod(lane, KRON) == mod(lax.broadcasted_iota(jnp.int32, (kron, 6 * kron), 0), KRON)
    which = div(lane, kron)
    total = jnp.zeros((kron, 6 * kron), F32)
    for k in range(3):
        tall = sum(lax.dot_general(up[t], pieces[t][k], (((1,), (1,)), ((), ())), preferred_element_type=F32)
                   for t in range(2)).astype(BF16)
        wide = jnp.dot(tall, across, preferred_element_type=F32)
        here = [n for n, kk in enumerate(kk for p, n2 in PASSES for kk in range(n2)) if kk == k]
        mask = same & functools.reduce(jnp.logical_or, [which == n for n in here])
        total = jnp.where(mask, wide, total)
    wk6[...] = total.astype(BF16)
    l_first.wait()
    l_split(1, nd - 1, l0)
    r_first.wait()
    r_split(1, nd - 1, r0)
    _, gmax = ar_wait(0)
    first_start((1.0 / vec(gmax)) * (2.0 ** -12))

    peers = {s: row_of(jnp.int32(s)) for s in (0, 1, 2, 4, 6)}

    def v_copy(src, slot, s):
        return pltpu.make_async_remote_copy(
            src_ref=vy.at[src], dst_ref=vy.at[slot], send_sem=vsend.at[slot], recv_sem=vrecv.at[slot],
            device_id={"row": peers[s]}, device_id_type=pl.DeviceIdType.MESH)

    def swap(a, b):
        a, b = a.reshape(-1, 8, a.shape[-1]), b.reshape(-1, 8, b.shape[-1])
        low = lax.broadcasted_iota(jnp.int32, a.shape, 1) < 4
        return jnp.where(low, a, pltpu.roll(b, 4, 1)), jnp.where(low, pltpu.roll(a, 4, 1), b)

    def t1_chunk(pieces, l, keep):
        got = six([pieces[k] for k in range(3)], [vp[p] for p in range(3)])
        for bh in range(2):
            both = swap(got[:, 2 * bh * ts:(2 * bh + 1) * ts], got[:, (2 * bh + 1) * ts:(2 * bh + 2) * ts])
            for e in range(2):
                at = (2 * l + e, slice(None), pl.ds(bh * ts, ts))
                t1[at] = jnp.where(keep, t1[at], 0.0) + both[e].reshape(ts, ts)

    def t1_group(g, carry):
        slot, a1, a2 = carry

        @pl.when(g > 0)
        def _():
            v_copy(0, g, 0).wait_recv()

        @pl.when((g > 0) & (mod(g, 2) == 0))
        def _():
            v_copy(g, g + 1, 1).start()

        for first, s in ((1, 4), (2, 6)):
            @pl.when(g == first)
            def _():
                v_copy(0, s, s).start()

        @pl.when(g < 7)
        def _():
            l_batch(1 - slot, a1, a2)

        l_batch_wait(slot)
        for n in range(4):
            for b in range(ts // SB):
                rows = pl.ds(b * SB, SB)
                for p, x in enumerate(split3(vy[g, n, rows, :])):
                    vp[p, rows, pl.ds(n * ts, ts)] = x
        for k in range(nd):
            l_split(slot, k, lps[(k + 1) % 2])
            t1_chunk(lps[k % 2], k, g > 0)
        return 1 - slot, a2, l_start(g + 3)

    t2_rows = min(64, hs)

    def t2_trip(i, carry):
        @pl.when(i == (hs // t2_rows))
        def _():
            r_batch(zero_i, r_start(zero_i), r_start(zero_i + 1))

        c0 = pl.multiple_of(i * t2_rows, t2_rows)
        for h in range(t2_rows // 8):
            for q in range(2):
                cols = pl.ds(q * ts, ts)
                x = t1[:, pl.ds(c0 + h * 8, 8), cols].reshape(nd, 2, 8, ts)
                parts = []
                for e in range(2):
                    b = split3(x[:, e].reshape(kron, ts))
                    rhs = jnp.concatenate([b[p] for p, n in PASSES for _ in range(n)], axis=0)
                    got = jnp.dot(wk6[...], rhs, preferred_element_type=F32)
                    parts.append(got.reshape(nd, 8, ts))
                for p, y in enumerate(split3(jnp.concatenate(parts, axis=1))):
                    t2[p, :, pl.ds(2 * c0 + h * 16, 16), cols] = y
        return carry

    def y_copy(src, idx, slot, to):
        return pltpu.make_async_remote_copy(
            src_ref=src, dst_ref=landing(slot), send_sem=ysend.at[idx], recv_sem=yrecv.at[slot],
            device_id={"col": to}, device_id_type=pl.DeviceIdType.MESH)

    def y_ref(dm, h):
        return vy.at[4 + dm, pl.ds(2 * h, 2)]

    def landing(slot):
        return recv.at[pl.ds(2 * slot, 2)]

    def add_into(dm, h, slot):
        y_copy(landing(slot), 0, slot, col).wait_recv()

        def add(i, c):
            n, rows = where_is(i)
            vy[4 + dm, 2 * h + n, rows, :] = vy[4 + dm, 2 * h + n, rows, :] + recv[2 * slot + n, rows, :]
            return c

        lax.fori_loop(0, nblk // 2, add, 0)

    def t3_chunk(pieces, r):
        return six([t2[k, r] for k in range(3)],
                   [pieces[k].reshape(2 * ts, ts) for k in range(3)])

    def t3_part(factor, i, carry):
        slot, d1, d2 = carry
        dm, h = block_of(i)

        @pl.when(i < 7)
        def _():
            r_batch(1 - slot, d1, d2)

        r_batch_wait(slot)
        total = None
        for k in range(nd):
            r_split(slot, k, rps[(k + 1) % 2])
            got = t3_chunk(rps[k % 2], k)
            total = got if total is None else total + got
        total = times(total, factor).reshape(ts // 8, 16, ts)
        for e, y in enumerate(swap(total[:, :8], total[:, 8:])):
            vy[4 + dm, 2 * h + e] = y.reshape(ts, ts)

        @pl.when(i == 2 * mz)
        def _():
            pl.semaphore_wait(fwd_ok, 1)

        @pl.when((mz == 1) & (i == 4))
        def _():
            pl.semaphore_wait(back_ok, 1)

        @pl.when((mz == 0) & (i < 6))
        def _():
            y_copy(y_ref(dm, h), i, i, col + zdir).start()

        @pl.when((mz == 1) & (i >= 2) & (i < 6))
        def _():
            k = i - 2
            add_into(3 - div(k, 2), mod(k, 2), k)
            y_copy(y_ref(3 - div(k, 2), mod(k, 2)), 6 + k, 6 + k, col + zdir).start()

        @pl.when((mz == 1) & (i >= 4) & (i < 6))
        def _():
            k = i - 4
            add_into(0, k, 6 + k)
            y_copy(y_ref(0, k), k, 6 + k, col - zdir).start()

        return 1 - slot, d2, r_start(i + 3)

    def step(j, state):
        gmax = state
        for s in (1, 2):
            v_copy(0, s, s).start()
        lax.fori_loop(0, 8, t1_group, (zero_i, l_start(zero_i + 1), l_start(zero_i + 2)))
        for s in range(1, 8):
            v_copy(0, s, 0).wait_send()

        @pl.when(mz == 0)
        def _():
            pl.semaphore_signal(back_ok, inc=1, device_id={"col": col + zdir}, device_id_type=pl.DeviceIdType.MESH)

        @pl.when(mz == 1)
        def _():
            pl.semaphore_signal(fwd_ok, inc=1, device_id={"col": col + zdir}, device_id_type=pl.DeviceIdType.MESH)
            pl.semaphore_signal(fwd_ok, inc=1, device_id={"col": col - zdir}, device_id_type=pl.DeviceIdType.MESH)

        total, _ = ar_wait(1)
        norm_v = jnp.sqrt(vec(total))
        inv = 1.0 / norm_v
        factor = vec(gmax) * inv * (2.0 ** 12)
        beta_prev = jnp.where(j > 0, norm_v, 0.0)
        norms[j] = norm_v

        lax.fori_loop(0, ts // t2_rows, t2_trip, 0)
        lax.fori_loop(0, 8, functools.partial(t3_part, factor), (zero_i, r_start(zero_i + 1), r_start(zero_i + 2)))

        own = 4 + mz
        near = 6 - 2 * mz
        for h in range(2):
            y_copy(landing(0), 0, near + h, col).wait_recv()

        @pl.when(mz == 0)
        def _():
            for k in range(6):
                y_copy(y_ref(0, 0), k, k, col).wait_send()

        @pl.when(mz == 1)
        def _():
            for h in range(2):
                y_copy(landing(0), 0, 8 + h, col).wait_recv()
            for k in (0, 1, 6, 7, 8, 9):
                y_copy(y_ref(0, 0), k, k, col).wait_send()

        def dots(i, c):
            n, rows = where_is(i)
            dot, mx = c
            w = vy[own, n, rows, :] + recv[2 * near + n, rows, :] + jnp.where(mz == 1, recv[16 + n, rows, :], 0.0)
            v = times(wprime[n, rows, :], inv)
            vcur[n, rows, :] = v
            wprime[n, rows, :] = w
            return dot + fold(jnp.add, v * w), jnp.maximum(mx, fold(jnp.maximum, jnp.abs(w)))

        zero = jnp.zeros((8, W8), F32)
        dot, mx = lax.fori_loop(0, nblk, dots, (zero, zero))
        ar_start(0, two_rows(as_row(dot, jnp.sum), as_row(mx, jnp.max)))

        @pl.when(j < STEPS - 1)
        def _():
            l_batch(zero_i, l_start(zero_i), l_start(zero_i + 1))

        alpha, gmax = ar_wait(0)
        out_ab[j] = alpha
        small = (1.0 / vec(gmax)) * (2.0 ** -12)

        def update(i, sq):
            n, rows = where_is(i)
            v = vcur[n, rows, :]
            x = wprime[n, rows, :] - alpha * v - times(vprev[n, rows, :], beta_prev)
            vprev[n, rows, :] = v
            wprime[n, rows, :] = x
            vy[0, n, rows, :] = times(x, small)
            return sq + fold(jnp.add, x * x)

        sq = lax.fori_loop(0, nblk, update, zero)
        ar_start(1, two_rows(as_row(sq, jnp.sum), jnp.zeros((1, 128), F32)))
        return gmax

    lax.fori_loop(0, STEPS, step, gmax)

    total, _ = ar_wait(1)
    norm_v = jnp.sqrt(vec(total))
    inv = 1.0 / norm_v
    norms[STEPS] = norm_v
    stores = [pltpu.make_async_copy(psi_v.at[b].reshape(ts, 2, LB), out_v.at[:, :, pl.ds(b * LB, LB)], iosem.at[b]) for b in blocks]
    for b, store in enumerate(stores):
        for sp in range(2):
            psi_v[b, pl.ds(sp, ts, stride=2), :] = times(
                wprime[2 * (b * LB // ts) + sp, :, pl.ds(b * LB % ts, LB)], inv)
        store.start()
    for j in range(STEPS):
        out_ab[STEPS + j] = jnp.max(norms[j + 1])
    for store in stores:
        store.wait()


def local_steps(ts, nd, psi_blk, left_blk, mpo_tensor, right_blk):
    lt = left_blk.transpose(1, 0, 2)
    rt = right_blk.transpose(1, 0, 2).reshape(4 * nd, ts // 2, 8 * ts)
    w_in = mpo_tensor.transpose(0, 2, 3, 1).reshape(2 * nd, 2, nd)
    any_space = pl.BlockSpec(memory_space=pl.ANY)
    dma, V = pltpu.SemaphoreType.DMA, pltpu.VMEM
    smem = pl.BlockSpec(memory_space=pltpu.SMEM)
    out_v, out_ab = pl.pallas_call(
        functools.partial(lanczos_kernel, ts, nd),
        out_shape=(jax.ShapeDtypeStruct((ts, 2, 2 * ts), F32), jax.ShapeDtypeStruct((2 * STEPS,), F32)),
        in_specs=[any_space] * 4,
        out_specs=(any_space, smem),
        scratch_shapes=[
            V((2 * ts // min(128, ts), 2 * ts, min(128, ts)), F32), V((2 * nd, 2, nd), F32), V((STEPS + 1, 8, min(128, ts)), F32),
            V((8, 4, ts, ts), F32), V((4, ts, ts), F32), V((4, ts, ts), F32), V((4, ts, ts), F32),
            V((max(20, 2 * nd), ts, ts), F32), V((2 * nd, ts, 2 * ts), F32), V((3, nd, 2 * ts, 2 * ts), BF16),
            V((3, ts, ts), BF16), V((3, ts, ts), BF16), V((3, 2, ts, ts), BF16), V((3, 2, ts, ts), BF16),
            V((3, ts, 4 * ts), BF16), V((2 * nd * KRON, 12 * nd * KRON), BF16),
            V((2, 2, 128), F32), V((2, NDEV, 2, 128), F32),
            dma((2,)), dma((2,)), dma((8,)), dma((8,)), dma((10,)), dma((10,)), dma((2,)), dma((2,)), dma((4,)), dma,
            pltpu.SemaphoreType.REGULAR, pltpu.SemaphoreType.REGULAR,
        ],
        compiler_params=pltpu.CompilerParams(vmem_limit_bytes=67043328, has_side_effects=True, collective_id=0),
    )(psi_blk, w_in, lt, rt)
    return out_ab[:STEPS], out_ab[STEPS:], out_v


def build(mesh, ts, nd):
    return jax.shard_map(
        functools.partial(local_steps, ts, nd), mesh=mesh,
        in_specs=(P("row", None, "col"), P("row", None, None), P(), P("col", None, None)),
        out_specs=(P(), P(), P("row", None, "col")), check_vma=False)


def solution(mesh):
    return build(mesh, 256, 14)
```

```python
import functools

import jax
import jax.numpy as jnp
from jax import lax
from jax.experimental import pallas as pl
from jax.experimental.pallas import tpu as pltpu
from jax.sharding import PartitionSpec as P

F32, BF16 = jnp.float32, jnp.bfloat16
STEPS = 4
NROW, NCOL = 8, 4
NDEV = NROW * NCOL
KRON = 4
PASSES = ((0, 3), (1, 2), (2, 1))


def div(a, b):
    return lax.div(a, jnp.int32(b))


def mod(a, b):
    return lax.rem(a, jnp.int32(b))


def split3(x):
    hi = x.astype(BF16)
    rest = x - hi.astype(F32)
    mid = rest.astype(BF16)
    low = (rest - mid.astype(F32)).astype(BF16)
    return hi, mid, low


def lanczos_kernel(ts, nd, psi, w_in, lt, rt, out_w, out_s,
                   psi_v, wv, norms, mults, vy, vcur, vprev, wprime, recv, t1, t2, l0, l1, r0, r1, vp, wk_a, wk_b, ar_src, ar_recv,
                   lsem, rsem, vsend, vrecv, ysend, yrecv, asend, arecv, iosem, wsem, fwd_ok, back_ok):
    row, col = lax.axis_index("row"), lax.axis_index("col")
    me = col * NROW + row
    core, xx, yy = mod(row, 2), mod(div(row, 2), 2), div(row, 4)
    hs = ts // 2
    kron = 2 * nd * KRON
    lps, rps = (l0, l1), (r0, r1)

    def six(lhs, rhs):
        a = [x for p, n in PASSES for x in lhs[:n]]
        b = [rhs[p] for p, n in PASSES for _ in range(n)]
        return jnp.dot(jnp.concatenate(a, axis=1), jnp.concatenate(b, axis=0), preferred_element_type=F32)

    def row_of(s):
        hi, two, odd = div(s, 4), mod(div(s, 2), 2), mod(s, 2)
        fp = (1 - hi) * two * (1 - odd) + hi * (two + (1 - two) * odd)
        fq = (1 - hi) * two * odd + hi * (two + (1 - two) * (1 - odd))
        fx, fy = (1 - core) * fp + core * fq, (1 - core) * fq + core * fp
        c2, x2, y2 = core + odd - 2 * core * odd, xx + fx - 2 * xx * fx, yy + fy - 2 * yy * fy
        return (y2 * 2 + x2) * 2 + c2

    half_z = div(col, 2)
    zdir = 1 - 2 * half_z
    mz = col + half_z * (3 - 2 * col)

    def block_of(i):
        late, two, odd = div(i, 4), div(i, 2), mod(i, 2)
        d_in = (1 - late) * 3 * (1 - odd) + late * (4 - two)
        h_in = (1 - late) * two + late * odd
        return (1 - mz) * (3 - two) + mz * d_in, (1 - mz) * odd + mz * h_in

    def l_start(g):
        return pl.multiple_of(row_of(mod(g, 8)) * ts, ts)

    def l_batch(slot, a0, a1):
        pltpu.make_async_copy(lt.at[pl.ds(1, nd - 1), :, pl.ds(pl.multiple_of(a0, ts), ts)],
                              recv.at[pl.ds(nd * slot, nd - 1)], lsem.at[slot]).start()
        pltpu.make_async_copy(lt.at[pl.ds(0, 1), :, pl.ds(pl.multiple_of(a1, ts), ts)],
                              recv.at[pl.ds(nd * slot + nd - 1, 1)], lsem.at[slot]).start()

    def l_batch_wait(slot):
        ref = recv.at[pl.ds(nd * slot, nd)]
        pltpu.make_async_copy(ref, ref, lsem.at[slot]).wait()

    def r_start(i):
        dm, h = block_of(mod(i, 8))
        dest = dm + half_z * (3 - 2 * dm)
        return pl.multiple_of((dest * 2 + h) * ts, ts)

    def r_rows(slot):
        return pl.ds(pl.multiple_of(slot * hs, hs), hs)

    half = nd // 2

    def r_batch(slot, d0, d1):
        for first, count, d, hh, plane in ((1, half, d0, 0, 0), (half + 1, half - 1, d0, 1, 0), (0, 1, d1, 1, 4 * half - 4)):
            if count:
                pltpu.make_async_copy(rt.at[pl.ds(4 * first, 4 * count), :, pl.ds(pl.multiple_of(d, ts), ts)],
                                      t1.at[pl.ds(plane, 4 * count), r_rows(slot), pl.ds(hh * ts, ts)],
                                      rsem.at[slot]).start()

    def r_batch_wait(slot):
        ref = t1.at[pl.ds(0, 4 * half), r_rows(slot)]
        pltpu.make_async_copy(ref, ref, rsem.at[slot]).wait()

    SB = min(32, ts)

    def l_split(slot, k, dst):
        for b in range(ts // SB):
            rows = pl.ds(b * SB, SB)
            for p, x in enumerate(split3(recv[nd * slot + k, rows, :])):
                dst[p, rows, :] = x

    def r_split(slot, k, dst):
        hh, kk = k // half, k % half
        sb = min(SB, hs)
        for kb in range(2):
            for bh in range(2):
                for b in range(hs // sb):
                    rows = pl.ds(pl.multiple_of(slot * hs + b * sb, sb), sb)
                    for p, x in enumerate(split3(t1[4 * kk + 2 * kb + bh, rows, pl.ds(hh * ts, ts)])):
                        dst[p, kb, pl.ds(bh * hs + b * sb, sb), :] = x

    def ar_start(slot, tile):
        ar_src[slot] = tile
        ar_recv[slot, me] = tile

        def send(off, carry):
            to = mod(me + off, NDEV)
            pltpu.make_async_remote_copy(
                src_ref=ar_src.at[slot], dst_ref=ar_recv.at[slot, me], send_sem=asend.at[slot], recv_sem=arecv.at[slot],
                device_id={"col": div(to, NROW), "row": mod(to, NROW)}, device_id_type=pl.DeviceIdType.MESH).start()
            return carry

        lax.fori_loop(1, NDEV, send, 0)

    def ar_wait(slot):
        every = ar_recv.at[slot, pl.ds(0, NDEV - 1)]
        copy = pltpu.make_async_remote_copy(
            src_ref=every, dst_ref=every, send_sem=asend.at[slot], recv_sem=arecv.at[slot],
            device_id={"col": col, "row": row}, device_id_type=pl.DeviceIdType.MESH)
        copy.wait_send()
        copy.wait_recv()

    def ar_read(slot):
        got = ar_recv[slot]
        total, most = jnp.sum(got, axis=0), jnp.max(got, axis=0)
        total = jnp.sum(total[0:1], axis=1, keepdims=True)
        most = jnp.max(most[1:2], axis=1, keepdims=True)
        return jnp.broadcast_to(total, (8, W8)), jnp.broadcast_to(most, (8, W8))

    W8 = min(128, ts)
    RB = min(64, ts)
    nblk = 4 * (ts // RB)

    def where_is(i):
        return div(i, ts // RB), pl.ds(pl.multiple_of(mod(i, ts // RB) * RB, RB), RB)

    def fold(op, x):
        x = x.reshape(-1, 8, ts)
        y = x[0]
        for k in range(1, x.shape[0]):
            y = op(y, x[k])
        if ts <= 128:
            return y
        return op(y[:, :128], y[:, 128:])

    def as_row(x, op):
        x = op(x, axis=0, keepdims=True)
        return x if W8 == 128 else jnp.concatenate([x, jnp.zeros((1, 128 - W8), F32)], axis=1)

    def two_rows(a, b):
        first = lax.broadcasted_iota(jnp.int32, (2, 128), 0) == 0
        return jnp.where(first, jnp.broadcast_to(a, (2, 128)), jnp.broadcast_to(b, (2, 128)))

    def times(x, v):
        wide = v if x.shape[-1] == v.shape[-1] else jnp.concatenate([v] * (x.shape[-1] // v.shape[-1]), axis=1)
        return (x.reshape(-1, 8, x.shape[-1]) * wide[None]).reshape(x.shape)

    def first_start(scale):
        def part(i, sq):
            n, rows = where_is(i)
            x = wprime[n, rows, :]
            vy[0, n, rows, :] = times(x, scale)
            return sq + fold(jnp.add, x * x)

        sq = lax.fori_loop(0, nblk, part, jnp.zeros((8, W8), F32))
        ar_start(1, two_rows(as_row(sq, jnp.sum), jnp.zeros((1, 128), F32)))

    barrier = pltpu.get_barrier_semaphore()

    def arrive(off, carry):
        to = mod(me + off, NDEV)
        pl.semaphore_signal(barrier, inc=1, device_id={"col": div(to, NROW), "row": mod(to, NROW)},
                            device_id_type=pl.DeviceIdType.MESH)
        return carry

    lax.fori_loop(1, NDEV, arrive, 0)
    LB = min(128, ts)
    blocks = range(2 * ts // LB)
    loads = [pltpu.make_async_copy(psi.at[:, :, pl.ds(b * LB, LB)], psi_v.at[b].reshape(ts, 2, LB), iosem.at[b]) for b in blocks]
    for load in loads:
        load.start()
    w_load = pltpu.make_async_copy(w_in, wv, wsem)
    w_load.start()
    l_first = pltpu.make_async_copy(lt.at[pl.ds(0, 1), :, pl.ds(pl.multiple_of(row * ts, ts), ts)],
                                    recv.at[pl.ds(2 * nd - 1, 1)], lsem.at[1])
    l_first.start()
    zero_i = jnp.int32(0)
    r_first = pltpu.make_async_copy(rt.at[pl.ds(0, 4), :, pl.ds(r_start(zero_i), ts)],
                                    t1.at[pl.ds(4 * half - 4, 4), r_rows(1), pl.ds(ts, ts)], rsem.at[1])
    r_first.start()
    l_batch(zero_i, l_start(zero_i), l_start(zero_i + 1))
    for b, load in enumerate(loads):
        load.wait()
        for sp in range(2):
            wprime[2 * (b * LB // ts) + sp, :, pl.ds(b * LB % ts, LB)] = psi_v[b, pl.ds(sp, ts, stride=2), :]

    def biggest(i, mx):
        n, rows = where_is(i)
        x = wprime[n, rows, :]
        vprev[n, rows, :] = jnp.zeros((RB, ts), F32)
        return jnp.maximum(mx, fold(jnp.maximum, jnp.abs(x)))

    mx = lax.fori_loop(0, nblk, biggest, jnp.zeros((8, W8), F32))
    pl.semaphore_wait(barrier, NDEV - 1)
    ar_start(0, two_rows(jnp.zeros((1, 128), F32), as_row(mx, jnp.max)))
    w_load.wait()
    pieces = [split3(wv[:, t, :]) for t in range(2)]
    at_row = lax.broadcasted_iota(jnp.int32, (kron, nd), 0)
    up = [((div(at_row, 2 * KRON) == lax.broadcasted_iota(jnp.int32, (kron, nd), 1)) & (mod(div(at_row, KRON), 2) == t))
          .astype(F32).astype(BF16) for t in range(2)]
    lane = lax.broadcasted_iota(jnp.int32, (2 * nd, 256), 1)
    across = ((div(mod(lane, kron), KRON) == lax.broadcasted_iota(jnp.int32, (2 * nd, 256), 0)) & (lane < 2 * kron))
    across = across.astype(F32).astype(BF16)
    lane = lax.broadcasted_iota(jnp.int32, (kron, 256), 1)
    same = mod(lane, KRON) == mod(lax.broadcasted_iota(jnp.int32, (kron, 256), 0), KRON)
    wide = []
    for k in range(3):
        tall = sum(lax.dot_general(up[t], pieces[t][k], (((1,), (1,)), ((), ())), preferred_element_type=F32)
                   for t in range(2)).astype(BF16)
        wide.append(jnp.where(same, jnp.dot(tall, across, preferred_element_type=F32), 0.0))
    for k in range(2):
        wk_a[pl.ds(k * kron, kron), :] = wide[k].astype(BF16)
    wk_b[...] = jnp.where(lane < kron, wide[2], wide[0]).astype(BF16)
    l_first.wait()
    l_split(1, nd - 1, l0)
    r_first.wait()
    r_split(1, nd - 1, r0)
    ar_wait(0)
    _, gmax = ar_read(0)
    first_start((1.0 / gmax) * (2.0 ** -12))

    peers = {s: row_of(jnp.int32(s)) for s in (0, 1, 2, 4, 6)}

    def v_copy(src, slot, s):
        return pltpu.make_async_remote_copy(
            src_ref=vy.at[src], dst_ref=vy.at[slot], send_sem=vsend.at[slot], recv_sem=vrecv.at[slot],
            device_id={"row": peers[s]}, device_id_type=pl.DeviceIdType.MESH)

    def swap(a, b):
        a, b = a.reshape(-1, 8, a.shape[-1]), b.reshape(-1, 8, b.shape[-1])
        low = lax.broadcasted_iota(jnp.int32, a.shape, 1) < 4
        return jnp.where(low, a, pltpu.roll(b, 4, 1)), jnp.where(low, pltpu.roll(a, 4, 1), b)

    def t1_chunk(pieces, l, keep):
        got = six([pieces[k] for k in range(3)], [vp[p] for p in range(3)])
        for bh in range(2):
            both = swap(got[:, 2 * bh * ts:(2 * bh + 1) * ts], got[:, (2 * bh + 1) * ts:(2 * bh + 2) * ts])
            for e in range(2):
                at = (2 * l + e, slice(None), pl.ds(bh * ts, ts))
                t1[at] = jnp.where(keep, t1[at], 0.0) + both[e].reshape(ts, ts)

    def t1_group(g, carry):
        slot, a1, a2 = carry

        @pl.when(g > 0)
        def _():
            v_copy(0, g, 0).wait_recv()

        @pl.when((g > 0) & (mod(g, 2) == 0))
        def _():
            v_copy(g, g + 1, 1).start()

        for first, s in ((1, 4), (2, 6)):
            @pl.when(g == first)
            def _():
                v_copy(0, s, s).start()

        @pl.when(g < 7)
        def _():
            l_batch(1 - slot, a1, a2)

        l_batch_wait(slot)
        for n in range(4):
            for b in range(ts // SB):
                rows = pl.ds(b * SB, SB)
                for p, x in enumerate(split3(vy[g, n, rows, :])):
                    vp[p, rows, pl.ds(n * ts, ts)] = x
        for k in range(nd):
            l_split(slot, k, lps[(k + 1) % 2])
            t1_chunk(lps[k % 2], k, g > 0)
        return 1 - slot, a2, l_start(g + 3)

    t2_rows = min(128, hs)

    def t2_trip(j, gmax, i, carry):
        @pl.when(i == (hs // t2_rows))
        def _():
            r_batch(zero_i, r_start(zero_i), r_start(zero_i + 1))

        norm = jnp.sqrt(ar_read(1)[0])
        inv = 1.0 / norm
        norms[j] = norm
        mults[0] = inv
        mults[1] = gmax * inv * (2.0 ** 12)
        c0 = pl.multiple_of(i * t2_rows, t2_rows)
        for h in range(t2_rows // 8):
            for q in range(2):
                cols = pl.ds(q * ts, ts)
                x = t1[:, pl.ds(c0 + h * 8, 8), cols].reshape(nd, 2, 8, ts)
                parts = []
                for e in range(2):
                    b = split3(x[:, e].reshape(kron, ts))
                    low = jnp.zeros((256 - 2 * kron, ts), BF16)
                    first = jnp.dot(wk_a[...], jnp.concatenate([b[0], b[1], low], axis=0), preferred_element_type=F32)
                    last = jnp.dot(wk_b[...], jnp.concatenate([b[0], b[2], low], axis=0), preferred_element_type=F32)
                    parts.append((first[:kron] + first[kron:] + last).reshape(nd, 8, ts))
                for p, y in enumerate(split3(jnp.concatenate(parts, axis=1))):
                    t2[p, :, pl.ds(2 * c0 + h * 16, 16), cols] = y
        return carry

    def y_copy(src, idx, slot, to):
        return pltpu.make_async_remote_copy(
            src_ref=src, dst_ref=landing(slot), send_sem=ysend.at[idx], recv_sem=yrecv.at[slot],
            device_id={"col": to}, device_id_type=pl.DeviceIdType.MESH)

    def y_ref(dm, h):
        return vy.at[4 + dm, pl.ds(2 * h, 2)]

    def landing(slot):
        return recv.at[pl.ds(2 * slot, 2)]

    def add_into(dm, h, slot):
        y_copy(landing(slot), 0, slot, col).wait_recv()

        for n in range(2):
            vy[4 + dm, 2 * h + n] = vy[4 + dm, 2 * h + n] + recv[2 * slot + n]

    def t3_part(i, carry):
        slot, d1, d2 = carry
        dm, h = block_of(i)

        @pl.when(i < 7)
        def _():
            r_batch(1 - slot, d1, d2)

        r_batch_wait(slot)
        total = [None, None]
        for k in range(nd):
            r_split(slot, k, rps[(k + 1) % 2])
            if k == 1:
                d3 = r_start(i + 3)
            for q in range(2):
                got = six([t2[p, k, pl.ds(q * ts, ts)] for p in range(3)],
                          [rps[k % 2][p].reshape(2 * ts, ts) for p in range(3)])
                total[q] = got if total[q] is None else total[q] + got
        for q in range(2):
            vy[4 + dm, 2 * h + q] = total[q]

        @pl.when(i == 2 * mz)
        def _():
            pl.semaphore_wait(fwd_ok, 1)

        @pl.when((mz == 1) & (i == 4))
        def _():
            pl.semaphore_wait(back_ok, 1)

        @pl.when((mz == 0) & (i < 6))
        def _():
            y_copy(y_ref(dm, h), i, i, col + zdir).start()

        @pl.when((mz == 1) & (i >= 2) & (i < 6))
        def _():
            k = i - 2
            add_into(3 - div(k, 2), mod(k, 2), k)
            y_copy(y_ref(3 - div(k, 2), mod(k, 2)), 6 + k, 6 + k, col + zdir).start()

        @pl.when((mz == 1) & (i >= 4) & (i < 6))
        def _():
            k = i - 4
            add_into(0, k, 6 + k)
            y_copy(y_ref(0, k), k, 6 + k, col - zdir).start()

        return 1 - slot, d2, d3

    def step(j, state):
        gmax = state
        for s in (1, 2):
            v_copy(0, s, s).start()
        lax.fori_loop(0, 8, t1_group, (zero_i, l_start(zero_i + 1), l_start(zero_i + 2)))
        for s in range(1, 8):
            v_copy(0, s, 0).wait_send()

        @pl.when(mz == 0)
        def _():
            pl.semaphore_signal(back_ok, inc=1, device_id={"col": col + zdir}, device_id_type=pl.DeviceIdType.MESH)

        @pl.when(mz == 1)
        def _():
            pl.semaphore_signal(fwd_ok, inc=1, device_id={"col": col + zdir}, device_id_type=pl.DeviceIdType.MESH)
            pl.semaphore_signal(fwd_ok, inc=1, device_id={"col": col - zdir}, device_id_type=pl.DeviceIdType.MESH)

        ar_wait(1)
        lax.fori_loop(0, ts // t2_rows, functools.partial(t2_trip, j, gmax), 0)
        lax.fori_loop(0, 8, t3_part, (zero_i, r_start(zero_i + 1), r_start(zero_i + 2)))

        own = 4 + mz
        near = 6 - 2 * mz
        for h in range(2):
            y_copy(landing(0), 0, near + h, col).wait_recv()

        @pl.when(mz == 0)
        def _():
            for k in range(6):
                y_copy(y_ref(0, 0), k, k, col).wait_send()

        @pl.when(mz == 1)
        def _():
            for h in range(2):
                y_copy(landing(0), 0, 8 + h, col).wait_recv()
            for k in (0, 1, 6, 7, 8, 9):
                y_copy(y_ref(0, 0), k, k, col).wait_send()

        inv, factor = mults[0], mults[1]
        CB = min(32, hs)

        def dots(i, c):
            dot, mx = c
            h, b = div(i, ts // CB), mod(i, ts // CB)
            n, rows = div(b, ts // (2 * CB)), pl.ds(pl.multiple_of(mod(b, ts // (2 * CB)) * 2 * CB, 2 * CB), 2 * CB)
            n = 2 * h + n
            y = vy[own, n, rows, :] + recv[2 * near + n, rows, :] + jnp.where(mz == 1, recv[16 + n, rows, :], 0.0)
            y = times(y, factor).reshape(CB // 8, 16, ts)
            at = pl.ds(pl.multiple_of(b * CB, CB), CB)
            for t, w in enumerate(swap(y[:, :8], y[:, 8:])):
                w = w.reshape(CB, ts)
                v = times(wprime[2 * h + t, at, :], inv)
                vcur[2 * h + t, at, :] = v
                wprime[2 * h + t, at, :] = w
                dot, mx = dot + fold(jnp.add, v * w), jnp.maximum(mx, fold(jnp.maximum, jnp.abs(w)))
            return dot, mx

        zero = jnp.zeros((8, W8), F32)
        dot, mx = lax.fori_loop(0, 2 * (ts // CB), dots, (zero, zero))
        ar_start(0, two_rows(as_row(dot, jnp.sum), as_row(mx, jnp.max)))

        @pl.when(j < STEPS - 1)
        def _():
            l_batch(zero_i, l_start(zero_i), l_start(zero_i + 1))

        ar_wait(0)
        alpha, gmax = ar_read(0)
        out_s[j] = alpha
        small = (1.0 / gmax) * (2.0 ** -12)
        beta_prev = jnp.where(j > 0, norms[j], 0.0)

        def update(i, sq):
            n, rows = where_is(i)
            v = vcur[n, rows, :]
            x = wprime[n, rows, :] - times(v, alpha) - times(vprev[n, rows, :], beta_prev)
            vprev[n, rows, :] = v
            wprime[n, rows, :] = x
            vy[0, n, rows, :] = times(x, small)
            return sq + fold(jnp.add, x * x)

        sq = lax.fori_loop(0, nblk, update, zero)
        ar_start(1, two_rows(as_row(sq, jnp.sum), jnp.zeros((1, 128), F32)))
        return gmax

    lax.fori_loop(0, STEPS, step, gmax)

    store = pltpu.make_async_copy(wprime, out_w, iosem.at[0])
    store.start()
    ar_wait(1)
    norms[STEPS] = jnp.sqrt(ar_read(1)[0])
    for j in range(STEPS):
        out_s[STEPS + j] = norms[j + 1]
    store.wait()


def last_kernel(ts, w, s, out_v, alpha, beta, psi_v, iosem):
    LB = min(128, ts)
    inv = 1.0 / s[2 * STEPS - 1][:, :LB]
    blocks = range(2 * ts // LB)
    stores = [pltpu.make_async_copy(psi_v.at[b].reshape(ts, 2, LB), out_v.at[:, :, pl.ds(b * LB, LB)], iosem.at[b]) for b in blocks]
    for b, store in enumerate(stores):
        for sp in range(2):
            x = w[2 * (b * LB // ts) + sp, :, pl.ds(b * LB % ts, LB)]
            psi_v[b, pl.ds(sp, ts, stride=2), :] = (x.reshape(ts // 8, 8, LB) * inv[None]).reshape(ts, LB)
        store.start()
    for j in range(STEPS):
        alpha[j] = jnp.max(s[j])
        beta[j] = jnp.max(s[STEPS + j])
    for store in stores:
        store.wait()


def local_steps(ts, nd, psi_blk, left_blk, mpo_tensor, right_blk):
    lt = left_blk.transpose(1, 0, 2)
    rt = right_blk.transpose(1, 0, 2).reshape(4 * nd, ts // 2, 8 * ts)
    w_in = mpo_tensor.transpose(0, 2, 3, 1).reshape(2 * nd, 2, nd)
    any_space = pl.BlockSpec(memory_space=pl.ANY)
    dma, V = pltpu.SemaphoreType.DMA, pltpu.VMEM
    smem = pl.BlockSpec(memory_space=pltpu.SMEM)
    vmem = pl.BlockSpec(memory_space=pltpu.VMEM)
    W8 = min(128, ts)
    out_w, out_s = pl.pallas_call(
        functools.partial(lanczos_kernel, ts, nd),
        out_shape=(jax.ShapeDtypeStruct((4, ts, ts), F32), jax.ShapeDtypeStruct((2 * STEPS, 8, W8), F32)),
        in_specs=[any_space] * 4,
        out_specs=(any_space, vmem),
        scratch_shapes=[
            V((2 * ts // min(128, ts), 2 * ts, min(128, ts)), F32), V((2 * nd, 2, nd), F32), V((STEPS + 1, 8, min(128, ts)), F32),
            V((2, 8, min(128, ts)), F32),
            V((8, 4, ts, ts), F32), V((4, ts, ts), F32), V((4, ts, ts), F32), V((4, ts, ts), F32),
            V((max(20, 2 * nd), ts, ts), F32), V((2 * nd, ts, 2 * ts), F32), V((3, nd, 2 * ts, 2 * ts), BF16),
            V((3, ts, ts), BF16), V((3, ts, ts), BF16), V((3, 2, ts, ts), BF16), V((3, 2, ts, ts), BF16),
            V((3, ts, 4 * ts), BF16), V((4 * nd * KRON, 256), BF16), V((2 * nd * KRON, 256), BF16),
            V((2, 2, 128), F32), V((2, NDEV, 2, 128), F32),
            dma((2,)), dma((2,)), dma((8,)), dma((8,)), dma((10,)), dma((10,)), dma((2,)), dma((2,)), dma((4,)), dma,
            pltpu.SemaphoreType.REGULAR, pltpu.SemaphoreType.REGULAR,
        ],
        compiler_params=pltpu.CompilerParams(vmem_limit_bytes=67043328, has_side_effects=True, collective_id=0),
    )(psi_blk, w_in, lt, rt)
    scalars = jax.ShapeDtypeStruct((STEPS,), F32)
    out_v, alpha, beta = pl.pallas_call(
        functools.partial(last_kernel, ts),
        out_shape=(jax.ShapeDtypeStruct((ts, 2, 2 * ts), F32), scalars, scalars),
        in_specs=[vmem, vmem],
        out_specs=(any_space, smem, smem),
        scratch_shapes=[V((2 * ts // W8, 2 * ts, W8), F32), dma((4,))],
        compiler_params=pltpu.CompilerParams(vmem_limit_bytes=8 << 20),
    )(out_w, out_s)
    return alpha, beta, out_v


def build(mesh, ts, nd):
    return jax.shard_map(
        functools.partial(local_steps, ts, nd), mesh=mesh,
        in_specs=(P("row", None, "col"), P("row", None, None), P(), P("col", None, None)),
        out_specs=(P(), P(), P("row", None, "col")), check_vma=False)


def solution(mesh):
    return build(mesh, 256, 14)
```

```python
import functools

import jax
import jax.numpy as jnp
from jax import lax
from jax.experimental import pallas as pl
from jax.experimental.pallas import tpu as pltpu
from jax.sharding import PartitionSpec as P

F32, BF16 = jnp.float32, jnp.bfloat16
STEPS = 4
NROW, NCOL = 8, 4
NDEV = NROW * NCOL
KRON = 4
PASSES = ((0, 3), (1, 2), (2, 1))


def div(a, b):
    return lax.div(a, jnp.int32(b))


def mod(a, b):
    return lax.rem(a, jnp.int32(b))


def split3(x):
    hi = x.astype(BF16)
    rest = x - hi.astype(F32)
    mid = rest.astype(BF16)
    low = (rest - mid.astype(F32)).astype(BF16)
    return hi, mid, low


def lanczos_kernel(ts, nd, psi, w_in, lt, rt, out_w, out_s,
                   psi_v, wv, norms, mults, vy, vcur, vprev, wprime, recv, t1, t2, l0, l1, r0, r1, l2, vp, wk_a, wk_b, ar_src, ar_recv,
                   lsem, rsem, vsend, vrecv, ysend, yrecv, asend, arecv, iosem, wsem, fwd_ok, back_ok):
    row, col = lax.axis_index("row"), lax.axis_index("col")
    me = col * NROW + row
    core, xx, yy = mod(row, 2), mod(div(row, 2), 2), div(row, 4)
    hs = ts // 2
    kron = 2 * nd * KRON
    lps, rps = (l0, l1, l2), (r0, r1)

    def six(lhs, rhs):
        a = [x for p, n in PASSES for x in lhs[:n]]
        b = [rhs[p] for p, n in PASSES for _ in range(n)]
        return jnp.dot(jnp.concatenate(a, axis=1), jnp.concatenate(b, axis=0), preferred_element_type=F32)

    def row_of(s):
        hi, two, odd = div(s, 4), mod(div(s, 2), 2), mod(s, 2)
        fp = (1 - hi) * two * (1 - odd) + hi * (two + (1 - two) * odd)
        fq = (1 - hi) * two * odd + hi * (two + (1 - two) * (1 - odd))
        fx, fy = (1 - core) * fp + core * fq, (1 - core) * fq + core * fp
        c2, x2, y2 = core + odd - 2 * core * odd, xx + fx - 2 * xx * fx, yy + fy - 2 * yy * fy
        return (y2 * 2 + x2) * 2 + c2

    half_z = div(col, 2)
    zdir = 1 - 2 * half_z
    mz = col + half_z * (3 - 2 * col)

    def block_of(i):
        late, two, odd = div(i, 4), div(i, 2), mod(i, 2)
        d_in = (1 - late) * 3 * (1 - odd) + late * (4 - two)
        h_in = (1 - late) * two + late * odd
        return (1 - mz) * (3 - two) + mz * d_in, (1 - mz) * odd + mz * h_in

    def l_start(g):
        return pl.multiple_of(row_of(mod(g, 8)) * ts, ts)

    def l_batch(slot, a0, a1):
        if nd > 2:
            pltpu.make_async_copy(lt.at[pl.ds(2, nd - 2), :, pl.ds(pl.multiple_of(a0, ts), ts)],
                                  recv.at[pl.ds(nd * slot, nd - 2)], lsem.at[slot]).start()
        pltpu.make_async_copy(lt.at[pl.ds(0, 2), :, pl.ds(pl.multiple_of(a1, ts), ts)],
                              recv.at[pl.ds(nd * slot + nd - 2, 2)], lsem.at[slot]).start()

    def l_batch_wait(slot):
        ref = recv.at[pl.ds(nd * slot, nd)]
        pltpu.make_async_copy(ref, ref, lsem.at[slot]).wait()

    def r_start(i):
        dm, h = block_of(mod(i, 8))
        dest = dm + half_z * (3 - 2 * dm)
        return pl.multiple_of((dest * 2 + h) * ts, ts)

    def r_rows(slot):
        return pl.ds(pl.multiple_of(slot * hs, hs), hs)

    half = nd // 2

    def r_batch(slot, d0, d1):
        for first, count, d, hh, plane in ((1, half, d0, 0, 0), (half + 1, half - 1, d0, 1, 0), (0, 1, d1, 1, 4 * half - 4)):
            if count:
                pltpu.make_async_copy(rt.at[pl.ds(4 * first, 4 * count), :, pl.ds(pl.multiple_of(d, ts), ts)],
                                      t1.at[pl.ds(plane, 4 * count), r_rows(slot), pl.ds(hh * ts, ts)],
                                      rsem.at[slot]).start()

    def r_batch_wait(slot):
        ref = t1.at[pl.ds(0, 4 * half), r_rows(slot)]
        pltpu.make_async_copy(ref, ref, rsem.at[slot]).wait()

    SB = min(32, ts)

    def l_split(slot, k, dst):
        for b in range(ts // SB):
            rows = pl.ds(b * SB, SB)
            for p, x in enumerate(split3(recv[nd * slot + k, rows, :])):
                dst[p, pl.ds(k % 2 * ts + b * SB, SB), :] = x

    def set_of(pair):
        return 0 if pair == 0 else 2 - pair % 2

    def r_split(slot, k, dst):
        hh, kk = k // half, k % half
        sb = min(SB, hs)
        for kb in range(2):
            for bh in range(2):
                for b in range(hs // sb):
                    rows = pl.ds(pl.multiple_of(slot * hs + b * sb, sb), sb)
                    for p, x in enumerate(split3(t1[4 * kk + 2 * kb + bh, rows, pl.ds(hh * ts, ts)])):
                        dst[p, kb, pl.ds(bh * hs + b * sb, sb), :] = x

    def ar_start(slot, tile):
        ar_src[slot] = tile
        ar_recv[slot, me] = tile

        def send(off, carry):
            to = mod(me + off, NDEV)
            pltpu.make_async_remote_copy(
                src_ref=ar_src.at[slot], dst_ref=ar_recv.at[slot, me], send_sem=asend.at[slot], recv_sem=arecv.at[slot],
                device_id={"col": div(to, NROW), "row": mod(to, NROW)}, device_id_type=pl.DeviceIdType.MESH).start()
            return carry

        lax.fori_loop(1, NDEV, send, 0)

    def ar_wait(slot):
        every = ar_recv.at[slot, pl.ds(0, NDEV - 1)]
        copy = pltpu.make_async_remote_copy(
            src_ref=every, dst_ref=every, send_sem=asend.at[slot], recv_sem=arecv.at[slot],
            device_id={"col": col, "row": row}, device_id_type=pl.DeviceIdType.MESH)
        copy.wait_send()
        copy.wait_recv()

    def ar_read(slot):
        got = ar_recv[slot]
        total, most = jnp.sum(got, axis=0), jnp.max(got, axis=0)
        total = jnp.sum(total[0:1], axis=1, keepdims=True)
        most = jnp.max(most[1:2], axis=1, keepdims=True)
        return jnp.broadcast_to(total, (8, W8)), jnp.broadcast_to(most, (8, W8))

    W8 = min(128, ts)
    RB = min(64, ts)
    nblk = 4 * (ts // RB)

    def where_is(i):
        return div(i, ts // RB), pl.ds(pl.multiple_of(mod(i, ts // RB) * RB, RB), RB)

    def fold(op, x):
        x = x.reshape(-1, 8, ts)
        y = x[0]
        for k in range(1, x.shape[0]):
            y = op(y, x[k])
        if ts <= 128:
            return y
        return op(y[:, :128], y[:, 128:])

    def as_row(x, op):
        x = op(x, axis=0, keepdims=True)
        return x if W8 == 128 else jnp.concatenate([x, jnp.zeros((1, 128 - W8), F32)], axis=1)

    def two_rows(a, b):
        first = lax.broadcasted_iota(jnp.int32, (2, 128), 0) == 0
        return jnp.where(first, jnp.broadcast_to(a, (2, 128)), jnp.broadcast_to(b, (2, 128)))

    def times(x, v):
        wide = v if x.shape[-1] == v.shape[-1] else jnp.concatenate([v] * (x.shape[-1] // v.shape[-1]), axis=1)
        return (x.reshape(-1, 8, x.shape[-1]) * wide[None]).reshape(x.shape)

    def first_start(scale):
        def part(i, sq):
            n, rows = where_is(i)
            x = wprime[n, rows, :]
            vy[0, n, rows, :] = times(x, scale)
            return sq + fold(jnp.add, x * x)

        sq = lax.fori_loop(0, nblk, part, jnp.zeros((8, W8), F32))
        ar_start(1, two_rows(as_row(sq, jnp.sum), jnp.zeros((1, 128), F32)))

    barrier = pltpu.get_barrier_semaphore()

    def arrive(off, carry):
        to = mod(me + off, NDEV)
        pl.semaphore_signal(barrier, inc=1, device_id={"col": div(to, NROW), "row": mod(to, NROW)},
                            device_id_type=pl.DeviceIdType.MESH)
        return carry

    lax.fori_loop(1, NDEV, arrive, 0)
    LB = min(128, ts)
    blocks = range(2 * ts // LB)
    loads = [pltpu.make_async_copy(psi.at[:, :, pl.ds(b * LB, LB)], psi_v.at[b].reshape(ts, 2, LB), iosem.at[b]) for b in blocks]
    for load in loads:
        load.start()
    w_load = pltpu.make_async_copy(w_in, wv, wsem)
    w_load.start()
    l_first = pltpu.make_async_copy(lt.at[pl.ds(0, 2), :, pl.ds(pl.multiple_of(row * ts, ts), ts)],
                                    recv.at[pl.ds(2 * nd - 2, 2)], lsem.at[1])
    l_first.start()
    zero_i = jnp.int32(0)
    r_first = pltpu.make_async_copy(rt.at[pl.ds(0, 4), :, pl.ds(r_start(zero_i), ts)],
                                    t1.at[pl.ds(4 * half - 4, 4), r_rows(1), pl.ds(ts, ts)], rsem.at[1])
    r_first.start()
    l_batch(zero_i, l_start(zero_i), l_start(zero_i + 1))
    for b, load in enumerate(loads):
        load.wait()
        for sp in range(2):
            wprime[2 * (b * LB // ts) + sp, :, pl.ds(b * LB % ts, LB)] = psi_v[b, pl.ds(sp, ts, stride=2), :]

    def biggest(i, mx):
        n, rows = where_is(i)
        x = wprime[n, rows, :]
        vprev[n, rows, :] = jnp.zeros((RB, ts), F32)
        return jnp.maximum(mx, fold(jnp.maximum, jnp.abs(x)))

    mx = lax.fori_loop(0, nblk, biggest, jnp.zeros((8, W8), F32))
    pl.semaphore_wait(barrier, NDEV - 1)
    ar_start(0, two_rows(jnp.zeros((1, 128), F32), as_row(mx, jnp.max)))
    w_load.wait()
    pieces = [split3(wv[:, t, :]) for t in range(2)]
    at_row = lax.broadcasted_iota(jnp.int32, (kron, nd), 0)
    up = [((div(at_row, 2 * KRON) == lax.broadcasted_iota(jnp.int32, (kron, nd), 1)) & (mod(div(at_row, KRON), 2) == t))
          .astype(F32).astype(BF16) for t in range(2)]
    lane = lax.broadcasted_iota(jnp.int32, (2 * nd, 256), 1)
    across = ((div(mod(lane, kron), KRON) == lax.broadcasted_iota(jnp.int32, (2 * nd, 256), 0)) & (lane < 2 * kron))
    across = across.astype(F32).astype(BF16)
    lane = lax.broadcasted_iota(jnp.int32, (kron, 256), 1)
    same = mod(lane, KRON) == mod(lax.broadcasted_iota(jnp.int32, (kron, 256), 0), KRON)
    wide = []
    for k in range(3):
        tall = sum(lax.dot_general(up[t], pieces[t][k], (((1,), (1,)), ((), ())), preferred_element_type=F32)
                   for t in range(2)).astype(BF16)
        wide.append(jnp.where(same, jnp.dot(tall, across, preferred_element_type=F32), 0.0))
    for k in range(2):
        wk_a[pl.ds(k * kron, kron), :] = wide[k].astype(BF16)
    wk_b[...] = jnp.where(lane < kron, wide[2], wide[0]).astype(BF16)
    l_first.wait()
    for k in range(2):
        l_split(1, nd - 2 + k, l0)
    r_first.wait()
    r_split(1, nd - 1, r0)
    ar_wait(0)
    _, gmax = ar_read(0)
    first_start((1.0 / gmax) * (2.0 ** -12))

    peers = {s: row_of(jnp.int32(s)) for s in (0, 1, 2, 4, 6)}

    def v_copy(src, slot, s):
        return pltpu.make_async_remote_copy(
            src_ref=vy.at[src], dst_ref=vy.at[slot], send_sem=vsend.at[slot], recv_sem=vrecv.at[slot],
            device_id={"row": peers[s]}, device_id_type=pl.DeviceIdType.MESH)

    def swap(a, b):
        a, b = a.reshape(-1, 8, a.shape[-1]), b.reshape(-1, 8, b.shape[-1])
        low = lax.broadcasted_iota(jnp.int32, a.shape, 1) < 4
        return jnp.where(low, a, pltpu.roll(b, 4, 1)), jnp.where(low, pltpu.roll(a, 4, 1), b)

    def t1_pair(pieces, pair, keep):
        got = six([pieces[k] for k in range(3)], [vp[p] for p in range(3)])
        for k in range(2):
            one = got[k * ts:(k + 1) * ts]
            for bh in range(2):
                both = swap(one[:, 2 * bh * ts:(2 * bh + 1) * ts], one[:, (2 * bh + 1) * ts:(2 * bh + 2) * ts])
                for e in range(2):
                    at = (4 * pair + 2 * k + e, slice(None), pl.ds(bh * ts, ts))
                    t1[at] = jnp.where(keep, t1[at], 0.0) + both[e].reshape(ts, ts)

    def t1_group(g, carry):
        slot, a1, a2 = carry

        @pl.when(g > 0)
        def _():
            v_copy(0, g, 0).wait_recv()

        @pl.when((g > 0) & (mod(g, 2) == 0))
        def _():
            v_copy(g, g + 1, 1).start()

        for first, s in ((1, 4), (2, 6)):
            @pl.when(g == first)
            def _():
                v_copy(0, s, s).start()

        @pl.when(g < 7)
        def _():
            l_batch(1 - slot, a1, a2)

        l_batch_wait(slot)
        for n in range(4):
            for b in range(ts // SB):
                rows = pl.ds(b * SB, SB)
                for p, x in enumerate(split3(vy[g, n, rows, :])):
                    vp[p, rows, pl.ds(n * ts, ts)] = x
        for pair in range(nd // 2):
            for k in range(2):
                l_split(slot, 2 * pair + k, lps[set_of((pair + 1) % (nd // 2))])
            t1_pair(lps[set_of(pair)], pair, g > 0)
        return 1 - slot, a2, l_start(g + 3)

    t2_rows = min(128, hs)

    def t2_trip(j, gmax, i, carry):
        @pl.when(i == (hs // t2_rows))
        def _():
            r_batch(zero_i, r_start(zero_i), r_start(zero_i + 1))

        norm = jnp.sqrt(ar_read(1)[0])
        inv = 1.0 / norm
        norms[j] = norm
        mults[0] = inv
        mults[1] = gmax * inv * (2.0 ** 12)
        c0 = pl.multiple_of(i * t2_rows, t2_rows)
        for h in range(t2_rows // 8):
            for q in range(2):
                cols = pl.ds(q * ts, ts)
                x = t1[:, pl.ds(c0 + h * 8, 8), cols].reshape(nd, 2, 8, ts)
                parts = []
                for e in range(2):
                    b = split3(x[:, e].reshape(kron, ts))
                    low = jnp.zeros((256 - 2 * kron, ts), BF16)
                    first = jnp.dot(wk_a[...], jnp.concatenate([b[0], b[1], low], axis=0), preferred_element_type=F32)
                    last = jnp.dot(wk_b[...], jnp.concatenate([b[0], b[2], low], axis=0), preferred_element_type=F32)
                    parts.append((first[:kron] + first[kron:] + last).reshape(nd, 8, ts))
                for p, y in enumerate(split3(jnp.concatenate(parts, axis=1))):
                    t2[p, :, pl.ds(2 * c0 + h * 16, 16), cols] = y
        return carry

    def y_copy(src, idx, slot, to):
        return pltpu.make_async_remote_copy(
            src_ref=src, dst_ref=landing(slot), send_sem=ysend.at[idx], recv_sem=yrecv.at[slot],
            device_id={"col": to}, device_id_type=pl.DeviceIdType.MESH)

    def y_ref(dm, h):
        return vy.at[4 + dm, pl.ds(2 * h, 2)]

    def landing(slot):
        return recv.at[pl.ds(2 * slot, 2)]

    def add_into(dm, h, slot):
        y_copy(landing(slot), 0, slot, col).wait_recv()

        for n in range(2):
            vy[4 + dm, 2 * h + n] = vy[4 + dm, 2 * h + n] + recv[2 * slot + n]

    def t3_part(i, carry):
        slot, d1, d2 = carry
        dm, h = block_of(i)

        @pl.when(i < 7)
        def _():
            r_batch(1 - slot, d1, d2)

        r_batch_wait(slot)
        total = None
        for k in range(nd):
            r_split(slot, k, rps[(k + 1) % 2])
            if k == 1:
                d3 = r_start(i + 3)
            got = six([t2[p, k] for p in range(3)], [rps[k % 2][p].reshape(2 * ts, ts) for p in range(3)])
            total = got if total is None else total + got
        vy[4 + dm, pl.ds(2 * h, 2)] = total.reshape(2, ts, ts)

        @pl.when(i == 2 * mz)
        def _():
            pl.semaphore_wait(fwd_ok, 1)

        @pl.when((mz == 1) & (i == 4))
        def _():
            pl.semaphore_wait(back_ok, 1)

        @pl.when((mz == 0) & (i < 6))
        def _():
            y_copy(y_ref(dm, h), i, i, col + zdir).start()

        @pl.when((mz == 1) & (i >= 2) & (i < 6))
        def _():
            k = i - 2
            add_into(3 - div(k, 2), mod(k, 2), k)
            y_copy(y_ref(3 - div(k, 2), mod(k, 2)), 6 + k, 6 + k, col + zdir).start()

        @pl.when((mz == 1) & (i >= 4) & (i < 6))
        def _():
            k = i - 4
            add_into(0, k, 6 + k)
            y_copy(y_ref(0, k), k, 6 + k, col - zdir).start()

        return 1 - slot, d2, d3

    def step(j, state):
        gmax = state
        for s in (1, 2):
            v_copy(0, s, s).start()
        lax.fori_loop(0, 8, t1_group, (zero_i, l_start(zero_i + 1), l_start(zero_i + 2)))
        for s in range(1, 8):
            v_copy(0, s, 0).wait_send()

        @pl.when(mz == 0)
        def _():
            pl.semaphore_signal(back_ok, inc=1, device_id={"col": col + zdir}, device_id_type=pl.DeviceIdType.MESH)

        @pl.when(mz == 1)
        def _():
            pl.semaphore_signal(fwd_ok, inc=1, device_id={"col": col + zdir}, device_id_type=pl.DeviceIdType.MESH)
            pl.semaphore_signal(fwd_ok, inc=1, device_id={"col": col - zdir}, device_id_type=pl.DeviceIdType.MESH)

        ar_wait(1)
        lax.fori_loop(0, ts // t2_rows, functools.partial(t2_trip, j, gmax), 0)
        lax.fori_loop(0, 8, t3_part, (zero_i, r_start(zero_i + 1), r_start(zero_i + 2)))

        own = 4 + mz
        near = 6 - 2 * mz
        for h in range(2):
            y_copy(landing(0), 0, near + h, col).wait_recv()

        @pl.when(mz == 0)
        def _():
            for k in range(6):
                y_copy(y_ref(0, 0), k, k, col).wait_send()

        @pl.when(mz == 1)
        def _():
            for h in range(2):
                y_copy(landing(0), 0, 8 + h, col).wait_recv()
            for k in (0, 1, 6, 7, 8, 9):
                y_copy(y_ref(0, 0), k, k, col).wait_send()

        inv, factor = mults[0], mults[1]
        CB = min(32, hs)

        def dots(i, c):
            dot, mx = c
            h, b = div(i, ts // CB), mod(i, ts // CB)
            n, rows = div(b, ts // (2 * CB)), pl.ds(pl.multiple_of(mod(b, ts // (2 * CB)) * 2 * CB, 2 * CB), 2 * CB)
            n = 2 * h + n
            y = vy[own, n, rows, :] + recv[2 * near + n, rows, :] + jnp.where(mz == 1, recv[16 + n, rows, :], 0.0)
            y = times(y, factor).reshape(CB // 8, 16, ts)
            at = pl.ds(pl.multiple_of(b * CB, CB), CB)
            for t, w in enumerate(swap(y[:, :8], y[:, 8:])):
                w = w.reshape(CB, ts)
                v = times(wprime[2 * h + t, at, :], inv)
                vcur[2 * h + t, at, :] = v
                wprime[2 * h + t, at, :] = w
                dot, mx = dot + fold(jnp.add, v * w), jnp.maximum(mx, fold(jnp.maximum, jnp.abs(w)))
            return dot, mx

        zero = jnp.zeros((8, W8), F32)
        dot, mx = lax.fori_loop(0, 2 * (ts // CB), dots, (zero, zero))
        ar_start(0, two_rows(as_row(dot, jnp.sum), as_row(mx, jnp.max)))

        @pl.when(j < STEPS - 1)
        def _():
            l_batch(zero_i, l_start(zero_i), l_start(zero_i + 1))

        ar_wait(0)
        alpha, gmax = ar_read(0)
        out_s[j] = alpha
        small = (1.0 / gmax) * (2.0 ** -12)
        beta_prev = jnp.where(j > 0, norms[j], 0.0)

        def update(i, sq):
            n, rows = where_is(i)
            v = vcur[n, rows, :]
            x = wprime[n, rows, :] - times(v, alpha) - times(vprev[n, rows, :], beta_prev)
            vprev[n, rows, :] = v
            wprime[n, rows, :] = x
            vy[0, n, rows, :] = times(x, small)
            return sq + fold(jnp.add, x * x)

        sq = lax.fori_loop(0, nblk, update, zero)
        ar_start(1, two_rows(as_row(sq, jnp.sum), jnp.zeros((1, 128), F32)))
        return gmax

    lax.fori_loop(0, STEPS, step, gmax)

    store = pltpu.make_async_copy(wprime, out_w, iosem.at[0])
    store.start()
    ar_wait(1)
    norms[STEPS] = jnp.sqrt(ar_read(1)[0])
    for j in range(STEPS):
        out_s[STEPS + j] = norms[j + 1]
    store.wait()


def last_kernel(ts, w, s, out_v, alpha, beta, psi_v, iosem):
    LB = min(128, ts)
    inv = 1.0 / s[2 * STEPS - 1][:, :LB]
    blocks = range(2 * ts // LB)
    stores = [pltpu.make_async_copy(psi_v.at[b].reshape(ts, 2, LB), out_v.at[:, :, pl.ds(b * LB, LB)], iosem.at[b]) for b in blocks]
    for b, store in enumerate(stores):
        for sp in range(2):
            x = w[2 * (b * LB // ts) + sp, :, pl.ds(b * LB % ts, LB)]
            psi_v[b, pl.ds(sp, ts, stride=2), :] = (x.reshape(ts // 8, 8, LB) * inv[None]).reshape(ts, LB)
        store.start()
    for j in range(STEPS):
        alpha[j] = jnp.max(s[j])
        beta[j] = jnp.max(s[STEPS + j])
    for store in stores:
        store.wait()


def local_steps(ts, nd, psi_blk, left_blk, mpo_tensor, right_blk):
    lt = left_blk.transpose(1, 0, 2)
    rt = right_blk.transpose(1, 0, 2).reshape(4 * nd, ts // 2, 8 * ts)
    w_in = mpo_tensor.transpose(0, 2, 3, 1).reshape(2 * nd, 2, nd)
    any_space = pl.BlockSpec(memory_space=pl.ANY)
    dma, V = pltpu.SemaphoreType.DMA, pltpu.VMEM
    smem = pl.BlockSpec(memory_space=pltpu.SMEM)
    vmem = pl.BlockSpec(memory_space=pltpu.VMEM)
    W8 = min(128, ts)
    out_w, out_s = pl.pallas_call(
        functools.partial(lanczos_kernel, ts, nd),
        out_shape=(jax.ShapeDtypeStruct((4, ts, ts), F32), jax.ShapeDtypeStruct((2 * STEPS, 8, W8), F32)),
        in_specs=[any_space] * 4,
        out_specs=(any_space, vmem),
        scratch_shapes=[
            V((2 * ts // min(128, ts), 2 * ts, min(128, ts)), F32), V((2 * nd, 2, nd), F32), V((STEPS + 1, 8, min(128, ts)), F32),
            V((2, 8, min(128, ts)), F32),
            V((8, 4, ts, ts), F32), V((4, ts, ts), F32), V((4, ts, ts), F32), V((4, ts, ts), F32),
            V((max(20, 2 * nd), ts, ts), F32), V((2 * nd, ts, 2 * ts), F32), V((3, nd, 2 * ts, 2 * ts), BF16),
            V((3, 2 * ts, ts), BF16), V((3, 2 * ts, ts), BF16), V((3, 2, ts, ts), BF16), V((3, 2, ts, ts), BF16),
            V((3, 2 * ts, ts), BF16),
            V((3, ts, 4 * ts), BF16), V((4 * nd * KRON, 256), BF16), V((2 * nd * KRON, 256), BF16),
            V((2, 2, 128), F32), V((2, NDEV, 2, 128), F32),
            dma((2,)), dma((2,)), dma((8,)), dma((8,)), dma((10,)), dma((10,)), dma((2,)), dma((2,)), dma((4,)), dma,
            pltpu.SemaphoreType.REGULAR, pltpu.SemaphoreType.REGULAR,
        ],
        compiler_params=pltpu.CompilerParams(vmem_limit_bytes=67043328, has_side_effects=True, collective_id=0),
    )(psi_blk, w_in, lt, rt)
    scalars = jax.ShapeDtypeStruct((STEPS,), F32)
    out_v, alpha, beta = pl.pallas_call(
        functools.partial(last_kernel, ts),
        out_shape=(jax.ShapeDtypeStruct((ts, 2, 2 * ts), F32), scalars, scalars),
        in_specs=[vmem, vmem],
        out_specs=(any_space, smem, smem),
        scratch_shapes=[V((2 * ts // W8, 2 * ts, W8), F32), dma((4,))],
        compiler_params=pltpu.CompilerParams(vmem_limit_bytes=8 << 20),
    )(out_w, out_s)
    return alpha, beta, out_v


def build(mesh, ts, nd):
    return jax.shard_map(
        functools.partial(local_steps, ts, nd), mesh=mesh,
        in_specs=(P("row", None, "col"), P("row", None, None), P(), P("col", None, None)),
        out_specs=(P(), P(), P("row", None, "col")), check_vma=False)


def solution(mesh):
    return build(mesh, 256, 14)
```
